32 devices in a mesh: groups: 2 (over y), cells: 4 (over z), obs: 2 (over x), mem: 2 (over core).
Axes of the slice: x: 2, y: 2, z: 4, core: 2. Of those that a mesh axis runs over, the one named last changes fastest.
Arguments:
- members: bfloat16 [64, 32768], P('mem', ('groups', 'cells', 'obs')), parts along dimension 1, may hold values from -4 to 4
- observed: float32 [16384], P(('groups', 'cells', 'obs')), parts along dimension 0, may hold values from -6 to 6
- obs_error: float32 [16384], P(('groups', 'cells', 'obs')), parts along dimension 0, may hold values from 0.25 to 2
- obs_cells: int32 [16384], P(('groups', 'cells', 'obs')), parts along dimension 0, may hold values from 0 to 2047
- perturbations: bfloat16 [16384, 64], P(('groups', 'cells', 'obs')), parts along dimension 0, may hold values from -5 to 5
- region_ids: int32 [64], P(('groups', 'cells', 'obs')), parts along dimension 0, may hold values from 0 to 3
Outputs:
- updated: bfloat16 [64, 32768], P('mem', ('groups', 'cells', 'obs')), parts along dimension 1
The draws below stay inside these ranges and needn't reach their ends.
There are 2 independent parts, one for each index of `groups`. The reference program is written for one: setup_inputs(seed, part) draws one part's arguments, and reference() takes and returns one part's arrays. A program takes and returns all parts, laid end to end along the dimension named above; each array names one. Nothing has to cross between parts.
Inputs may be any that keep to these rules, and one draw needn't show every extreme that they name: obs_cells[j] names a cell of section j // 1024, the cells s * 2048 to (s + 1) * 2048 - 1 forming section s. `region_ids`: block b holds the cells b * 512 to (b + 1) * 512 - 1.
All inputs are finite; a program needn't handle non-finite values.
Results may differ from the reference program's by a relative error of at most 0.006.
Values may be sent and summed in bfloat16 or wider, within the bound.
No kernel may reach another device: no remote copies, remote signals or barrier semaphores. Data moves between devices by JAX's collectives and lax.ppermute only.
A program may use at most 64 MiB of HBM per device.

```python
import jax
import jax.numpy as jnp

NE = 64
CELL_DEV = 2048
OBS_DEV = 1024
BLOCK = 512
NLOC = 4
ITERS = 1
CELLS = 16384
NOBS = 8192
NBLK = 32


def draw_obs_error(key, part):
    position = jnp.arange(NOBS, dtype=jnp.float32) / NOBS
    trend = jnp.exp(-0.5 * jnp.log(3.0) * position)
    rough = jnp.exp(jax.random.uniform(key, (NOBS,), jnp.float32, jnp.log(0.5), jnp.log(2.0)))
    return (rough * trend).astype(jnp.float32)


def plant(drawn, key, least, largest):
    longest = drawn.shape.index(max(drawn.shape))
    spots = []
    for shift in (0, 1):
        where = [jax.random.randint(jax.random.fold_in(key, axis), (), 0, length) for axis, length in enumerate(drawn.shape)]
        where[longest] = (where[longest] + shift) % drawn.shape[longest]
        spots.append(tuple(where))
    return drawn.at[spots[0]].set(least).at[spots[1]].set(largest)


def level_of(own_key, dims, split, low, high):
    factor_of, own = 1.0, jax.random.fold_in(own_key, 6)
    for dim, shards_of in split:
        draws = jnp.exp(jax.random.uniform(jax.random.fold_in(own, dim), (shards_of,), jnp.float32, low / len(split), high / len(split)))
        factor_of = factor_of * jnp.repeat(draws, dims[dim] // shards_of).reshape([-1 if axis == dim else 1 for axis in range(len(dims))])
    return factor_of


def normal_values(key, dims, spread, bound, shards=(), held_as=jnp.bfloat16):
    drawn = spread * jax.random.normal(key, dims, jnp.float32)
    if shards:
        drawn = drawn * level_of(key, dims, shards, -0.22, 0.18)
    return jnp.clip(drawn, -bound, bound).astype(held_as)


def setup_inputs(seed: int = 0, part: int = 0) -> dict:
    streams_of = jax.random.split(jax.random.key(seed), 7)
    own_keys = jax.random.split(jax.random.fold_in(streams_of[6], part), 7)
    members = normal_values(own_keys[0], (NE, CELLS), 1.0, 4.0, ((0, 2), (1, 8)))
    observed = normal_values(own_keys[1], (NOBS,), 1.5, 6.0, ((0, 8),), jnp.float32)
    obs_error = draw_obs_error(jax.random.fold_in(jax.random.fold_in(streams_of[6], part), 71), part)
    obs_cells = plant(jax.random.randint(own_keys[3], (NOBS,), 0, CELL_DEV), jax.random.fold_in(own_keys[3], 1), 0, CELL_DEV - 1).astype(jnp.int32)
    perturbations = normal_values(own_keys[4], (NOBS, NE), 1.0, 5.0, ((0, 8),))
    region_ids = plant(jax.random.randint(own_keys[5], (NBLK,), 0, NLOC), jax.random.fold_in(own_keys[5], 1), 0, NLOC - 1).astype(jnp.int32)
    return dict(members=members, observed=observed, obs_error=obs_error, obs_cells=obs_cells, perturbations=perturbations, region_ids=region_ids)


def solve_regions(gram, cross, misfit):
    damping = NE - 1.0 + misfit / NE
    eye = jnp.eye(NE, dtype=gram.dtype)
    system = gram + damping[:, None, None] * eye[None, :, :]
    factor = jnp.linalg.cholesky(system)
    return jax.vmap(lambda fac, rhs: jax.scipy.linalg.cho_solve((fac, True), rhs))(factor, cross)

def reference(members, observed, obs_error, obs_cells, perturbations, region_ids):
    cell_index = jnp.arange(NOBS, dtype=jnp.int32) // OBS_DEV * CELL_DEV + obs_cells.astype(jnp.int32)
    cell_region = jnp.repeat(region_ids, BLOCK)
    obs_region = cell_region[cell_index]
    ensemble = members.T
    for step in range(ITERS):
        center = jnp.sum(ensemble.astype(jnp.float32), axis=1) / NE
        anomaly = (ensemble.astype(jnp.float32) - center[:, None]).astype(jnp.bfloat16)
        values = ensemble[cell_index].astype(jnp.float32)
        predicted = values + 0.2 * values * values * values
        pmean = jnp.sum(predicted, axis=1) / NE
        sens = ((predicted - pmean[:, None]) / obs_error[:, None]).astype(jnp.bfloat16)
        innov = (observed[:, None] - predicted) / obs_error[:, None] + perturbations.astype(jnp.float32)
        innov_b = innov.astype(jnp.bfloat16)
        joined = jnp.concatenate([sens, innov_b], axis=1)
        grams = []
        misfits = []
        for region in range(NLOC):
            inside = obs_region == region
            masked = jnp.where(inside[:, None], sens, jnp.zeros_like(sens))
            grams.append(jnp.dot(masked.T.astype(jnp.float32), joined.astype(jnp.float32), preferred_element_type=jnp.float32))
            misfits.append(jnp.sum(jnp.where(inside[:, None], innov * innov, jnp.float32(0.0))))
        stacked = jnp.stack(grams)
        misfit = jnp.stack(misfits)
        coeff = solve_regions(stacked[:, :, :NE], stacked[:, :, NE:], misfit).astype(jnp.bfloat16)
        delta = jnp.zeros(ensemble.shape, jnp.float32)
        for region in range(NLOC):
            product = jnp.dot(anomaly.astype(jnp.float32), coeff[region].astype(jnp.float32), preferred_element_type=jnp.float32)
            delta = delta + jnp.where((cell_region == region)[:, None], product, jnp.float32(0.0))
        ensemble = (ensemble.astype(jnp.float32) + delta).astype(jnp.bfloat16)
    return ensemble.T
```

```python
import functools

import jax
import jax.numpy as jnp
from jax import lax
from jax.experimental import pallas as pl
from jax.experimental.pallas import tpu as pltpu
from jax.sharding import PartitionSpec as P

NLOC = 4
BLOCK = 512
SUB = 8
LANES = 128
TILE = 256


VMEM = pl.BlockSpec(memory_space=pltpu.VMEM)
SMEM = pl.BlockSpec(memory_space=pltpu.SMEM)


def in_order(mine, theirs):
    first = lax.axis_index("mem") == 0
    return jnp.where(first, mine, theirs), jnp.where(first, theirs, mine)


def stats_kernel(mine_ref, theirs_ref, observed_ref, error_ref, cells_ref, noise_ref, regions_ref, out_ref):
    half, cells = mine_ref.shape
    ne = 2 * half
    nobs = observed_ref.shape[1]
    low, high = in_order(mine_ref[...], theirs_ref[...])
    whole = jnp.concatenate([low, high], axis=0)
    cell = cells_ref[...]
    part = cell // TILE
    within = cell - part * TILE
    onehot = (lax.broadcasted_iota(jnp.int32, (TILE, nobs), 0) == within).astype(jnp.bfloat16)
    values = jnp.zeros((ne, nobs), jnp.float32)
    for p in range(cells // TILE):
        picked = jnp.dot(
            whole[:, p * TILE : (p + 1) * TILE], onehot, preferred_element_type=jnp.float32
        )
        values = jnp.where(part == p, picked, values)
    predicted = values + 0.2 * values * values * values
    pmean = jnp.sum(predicted, axis=0, keepdims=True) / ne
    error = error_ref[...]
    sens = ((predicted - pmean) / error).astype(jnp.bfloat16)
    innov = (observed_ref[...] - predicted) / error + noise_ref[...].astype(jnp.float32)
    innov_b = innov.astype(jnp.bfloat16)
    square = jnp.sum(innov * innov, axis=0, keepdims=True)
    block = cell // BLOCK
    region = jnp.zeros_like(cell)
    for b in range(cells // BLOCK):
        region = jnp.where(block == b, regions_ref[b], region)
    base = lax.axis_index("mem") * 2
    inside = [region == base + r for r in range(2)]
    zero = jnp.zeros_like(sens)
    masked = jnp.concatenate([jnp.where(m, sens, zero) for m in inside], axis=0)
    joined = jnp.concatenate([sens, innov_b, innov_b, sens], axis=0)
    sums = lax.dot_general(
        masked, joined, (((1,), (1,)), ((), ())), preferred_element_type=jnp.float32
    )
    out_ref[0:ne, :] = sums[0:ne, 0 : 2 * ne]
    out_ref[ne : 2 * ne, :] = sums[ne : 2 * ne, 2 * ne : 4 * ne]
    rows = []
    for m in inside:
        kept = jnp.where(m, square, jnp.float32(0.0))
        rows.append(
            functools.reduce(
                jnp.add, [kept[:, i * LANES : (i + 1) * LANES] for i in range(nobs // LANES)]
            )
        )
    out_ref[2 * ne : 2 * ne + SUB, :] = jnp.concatenate(
        rows + [jnp.zeros((SUB - 2, LANES), jnp.float32)], axis=0
    )


def row_of(x, j):
    return jnp.broadcast_to(x[j : j + 1, :], x.shape)


def lane_of(x, c):
    return jnp.broadcast_to(x[:, c : c + 1], x.shape)


def eliminate(systems, offsets):
    count = len(systems)
    blocks = len(systems[0])
    sub = lax.broadcasted_iota(jnp.int32, (SUB, LANES), 0)
    for k in range(blocks):
        cols = [
            [[lane_of(systems[s][i], offsets[s] + SUB * k + j) for j in range(SUB)] for i in range(blocks)]
            for s in range(count)
        ]
        panel = [systems[s][k] for s in range(count)]
        diag = [list(cols[s][k]) for s in range(count)]
        for j in range(SUB):
            for s in range(count):
                d = diag[s][j]
                inverse = 1.0 / row_of(d, j)
                rest = jnp.where(sub == j, 0.0, d)
                for l in range(j + 1, SUB):
                    row = row_of(diag[s][l], j) * inverse
                    diag[s][l] = jnp.where(sub == j, row, diag[s][l] - rest * row)
                row = row_of(panel[s], j) * inverse
                panel[s] = jnp.where(sub == j, row, panel[s] - rest * row)
        for s in range(count):
            for i in range(blocks):
                if i == k:
                    continue
                x = systems[s][i]
                for j in range(SUB):
                    x = x - cols[s][i][j] * row_of(panel[s], j)
                systems[s][i] = x
            systems[s][k] = panel[s]
    return systems


def solve_kernel(*refs):
    *shares, mine_ref, theirs_ref = refs
    total = functools.reduce(jnp.add, [s[...] for s in shares])
    ne = (total.shape[0] - SUB) // 2
    lane = lax.broadcasted_iota(jnp.int32, (SUB, LANES), 1)
    sub = lax.broadcasted_iota(jnp.int32, (SUB, LANES), 0)
    tail = total[2 * ne : 2 * ne + SUB]
    misfit = jnp.sum(tail, axis=1, keepdims=True)
    damping = (ne - 1.0) + misfit / ne
    systems = []
    offsets = (0, ne)
    for s in range(2):
        d = jnp.broadcast_to(damping[s : s + 1, :], (SUB, LANES))
        rows = []
        for i in range(ne // SUB):
            x = total[s * ne + i * SUB : s * ne + (i + 1) * SUB]
            rows.append(jnp.where(lane == offsets[s] + SUB * i + sub, x + d, x))
        systems.append(rows)
    first, second = eliminate(systems, offsets)
    both = jnp.concatenate(
        [jnp.where(lane < ne, b, a) for a, b in zip(first, second)], axis=0
    )
    turned = both.T.astype(jnp.bfloat16)
    half = ne // 2
    quarter = [turned[q * half : (q + 1) * half] for q in range(4)]
    low = jnp.concatenate([quarter[2], quarter[0]], axis=0)
    high = jnp.concatenate([quarter[3], quarter[1]], axis=0)
    first = lax.axis_index("mem") == 0
    mine_ref[...] = jnp.where(first, low, high)
    theirs_ref[...] = jnp.where(first, high, low)


def anomaly_kernel(mine_ref, theirs_ref, out_ref):
    low, high = in_order(mine_ref[...], theirs_ref[...])
    whole = jnp.concatenate([low, high], axis=0).astype(jnp.float32)
    center = jnp.sum(whole, axis=0, keepdims=True) / whole.shape[0]
    out_ref[...] = (whole - center).astype(jnp.bfloat16)


def apply_kernel(mine_ref, theirs_ref, anomaly_ref, members_ref, regions_ref, out_ref, coeff_ref):
    half = members_ref.shape[0]
    rows = mine_ref.shape[0]
    coeff_ref[0:rows, :] = mine_ref[...]
    coeff_ref[rows : 2 * rows, :] = theirs_ref[...]
    core = lax.axis_index("mem")
    for b in range(members_ref.shape[1] // BLOCK):
        region = regions_ref[b]
        start = jnp.where(region // 2 == core, 0, rows) + (region % 2) * half
        coeff = coeff_ref[pl.ds(pl.multiple_of(start, half), half), :]
        span = slice(b * BLOCK, (b + 1) * BLOCK)
        delta = jnp.dot(coeff, anomaly_ref[:, span], preferred_element_type=jnp.float32)
        out_ref[:, span] = (members_ref[:, span].astype(jnp.float32) + delta).astype(jnp.bfloat16)


def exchanges(x, axis):
    size = lax.axis_size(axis)
    if size & (size - 1):
        return [lax.psum(x, axis)]
    parts, step = [x], 1
    while step < size:
        width = 4 if size // step >= 4 else 2
        x = functools.reduce(jnp.add, parts)
        parts = [x] + [
            lax.ppermute(x, axis, [(i, i ^ (m * step)) for i in range(size)]) for m in range(1, width)
        ]
        step *= width
    return parts


def body(members, observed, obs_error, obs_cells, perturbations, region_ids):
    half, cells = members.shape
    ne = 2 * half
    nobs = observed.shape[0]
    swap = [(0, 1), (1, 0)]
    other = lax.ppermute(members, "mem", swap)
    sums = pl.pallas_call(
        stats_kernel,
        out_shape=jax.ShapeDtypeStruct((2 * ne + SUB, 2 * ne), jnp.float32),
        in_specs=[VMEM] * 6 + [SMEM],
        out_specs=VMEM,
        name="stats",
    )(
        members,
        other,
        observed.reshape(1, nobs),
        obs_error.reshape(1, nobs),
        obs_cells.reshape(1, nobs),
        perturbations.T,
        region_ids,
    )
    sums = functools.reduce(jnp.add, exchanges(sums, "obs"))
    shares = exchanges(sums, "cells")
    anomaly = pl.pallas_call(
        anomaly_kernel,
        out_shape=jax.ShapeDtypeStruct((ne, cells), jnp.bfloat16),
        in_specs=[VMEM] * 2,
        out_specs=VMEM,
        name="anomaly",
    )(members, other)
    mine, theirs = pl.pallas_call(
        solve_kernel,
        out_shape=[jax.ShapeDtypeStruct((ne, ne), jnp.bfloat16)] * 2,
        in_specs=[VMEM] * len(shares),
        out_specs=[VMEM] * 2,
        name="solve",
    )(*shares)
    theirs = lax.ppermute(theirs, "mem", swap)
    return pl.pallas_call(
        apply_kernel,
        out_shape=jax.ShapeDtypeStruct((half, cells), jnp.bfloat16),
        in_specs=[VMEM] * 4 + [SMEM],
        out_specs=VMEM,
        scratch_shapes=[pltpu.VMEM((2 * ne, ne), jnp.bfloat16)],
        name="apply",
    )(mine, theirs, anomaly, members, region_ids)


def solution(mesh):
    cut = ("groups", "cells", "obs")
    in_specs = (P("mem", cut), P(cut), P(cut), P(cut), P(cut, None), P(cut))
    return jax.shard_map(
        body, mesh=mesh, in_specs=in_specs, out_specs=P("mem", cut), check_vma=False
    )
```

```python
import functools

import jax
import jax.numpy as jnp
from jax import lax
from jax.experimental import pallas as pl
from jax.experimental.pallas import tpu as pltpu
from jax.sharding import PartitionSpec as P

NLOC = 4
BLOCK = 512
SUB = 8
LANES = 128
TILE = 256


VMEM = pl.BlockSpec(memory_space=pltpu.VMEM)
SMEM = pl.BlockSpec(memory_space=pltpu.SMEM)
HBM = pl.BlockSpec(memory_space=pl.ANY)


def near(x):
    return pltpu.with_memory_space_constraint(x, pltpu.VMEM)


def prepare_kernel(
    members_hbm, cells_hbm, observed_hbm, error_hbm, noise_hbm, regions_ref,
    members_ref, onehot_ref, predicted_ref, innov_ref, noise_ref, rows_ref, cells_ref, observed_ref,
    error_ref, all_noise_ref, sems,
):
    moves = [
        pltpu.make_async_copy(src, dst, sems.at[i])
        for i, (src, dst) in enumerate(
            (
                (cells_hbm, cells_ref),
                (members_hbm, members_ref),
                (error_hbm, error_ref),
                (observed_hbm, observed_ref),
                (noise_hbm, all_noise_ref),
            )
        )
    ]
    for move in moves:
        move.start()
    half, cells = members_ref.shape
    nobs = cells_ref.shape[1]
    moves[0].wait()
    cell = cells_ref[...]
    part = cell // TILE
    block = cell // BLOCK
    region = jnp.zeros_like(cell)
    for b in range(cells // BLOCK):
        region = jnp.where(block == b, regions_ref[b], region)
    onehot = lax.broadcasted_iota(jnp.int32, (TILE, nobs), 0) == cell - part * TILE
    onehot = onehot.astype(jnp.bfloat16)
    onehot_ref[...] = onehot
    moves[1].wait()
    predicted = predict(members_ref, onehot, part)
    predicted_ref[...] = predicted
    moves[2].wait()
    moves[3].wait()
    inverse = 1.0 / error_ref[...]
    moves[4].wait()
    core = lax.axis_index("mem")
    noise = all_noise_ref[pl.ds(pl.multiple_of(core * half, half), half), :].astype(jnp.float32)
    innov = (observed_ref[...] - predicted) * inverse + noise
    innov_ref[...] = innov.astype(jnp.bfloat16)
    noise_ref[...] = all_noise_ref[pl.ds(pl.multiple_of((1 - core) * half, half), half), :]
    rows_ref[0:1, :] = observed_ref[...]
    rows_ref[1:2, :] = inverse
    rows_ref[2:3, :] = part.astype(jnp.float32)
    rows_ref[3:4, :] = (region - 2 * core).astype(jnp.float32)
    rows_ref[4:5, :] = jnp.sum(predicted, axis=0, keepdims=True)
    rows_ref[5:6, :] = jnp.sum(innov * innov, axis=0, keepdims=True)
    rows_ref[6:8, :] = jnp.zeros((2, nobs), jnp.float32)


def predict(members_ref, onehot, part):
    members, cells = members_ref.shape
    values = jnp.zeros((members, part.shape[1]), jnp.float32)
    for p in range(cells // TILE):
        picked = jnp.dot(
            members_ref[:, p * TILE : (p + 1) * TILE], onehot, preferred_element_type=jnp.float32
        )
        values = jnp.where(part == p, picked, values)
    return values + 0.2 * values * values * values


def stats_kernel(theirs_ref, onehot_ref, predicted_ref, innov_ref, noise_ref, rows_ref, out_ref):
    half = theirs_ref.shape[0]
    ne = 2 * half
    observed, inverse, part, region, mine_sum, mine_square = [rows_ref[i : i + 1, :] for i in range(6)]
    mine = predicted_ref[...]
    theirs = predict(theirs_ref, onehot_ref[...], part)
    innov = (observed - theirs) * inverse + noise_ref[...].astype(jnp.float32)
    square = mine_square + jnp.sum(innov * innov, axis=0, keepdims=True)
    pmean = (mine_sum + jnp.sum(theirs, axis=0, keepdims=True)) / ne
    sens = jnp.concatenate(
        [((mine - pmean) * inverse).astype(jnp.bfloat16), ((theirs - pmean) * inverse).astype(jnp.bfloat16)], axis=0
    )
    innov_b = jnp.concatenate([innov_ref[...], innov.astype(jnp.bfloat16)], axis=0)
    inside = [region == r for r in (0.0, 1.0)]
    zero = jnp.zeros_like(sens)
    masked = jnp.concatenate([jnp.where(m, x, zero) for x in (sens, innov_b) for m in inside], axis=0)
    sums = lax.dot_general(
        sens, masked, (((1,), (1,)), ((), ())), preferred_element_type=jnp.float32
    )
    out_ref[0:ne, :] = sums[:, 0 : 2 * ne]
    out_ref[ne : 2 * ne, :] = sums[:, 2 * ne : 4 * ne]
    first, second = [
        jnp.sum(jnp.where(m, square, jnp.float32(0.0)), axis=1, keepdims=True) for m in inside
    ]
    lane = lax.broadcasted_iota(jnp.int32, (SUB, LANES), 1)
    out_ref[2 * ne : 2 * ne + SUB, :] = jnp.where(lane < ne, first, second)


def row_of(x, j):
    return jnp.broadcast_to(x[j : j + 1, :], x.shape)


def lane_of(x, c, lane):
    half = LANES // 2
    index = jnp.where(lane < half, c, half + c)
    return jnp.take_along_axis(x, index, axis=1, mode="promise_in_bounds")


def eliminate(left, right):
    blocks = len(left)
    sub = lax.broadcasted_iota(jnp.int32, (SUB, LANES), 0)
    lane = lax.broadcasted_iota(jnp.int32, (SUB, LANES), 1)
    for k in range(blocks):
        cols = [[lane_of(left[i], SUB * k + j, lane) for i in range(blocks)] for j in range(SUB)]
        diag = [cols[j][k] for j in range(SUB)]
        panel = [left[k], right[k]]
        for j in range(SUB):
            inverse = 1.0 / row_of(diag[j], j)
            rest = jnp.where(sub == j, 0.0, diag[j])
            for values, start in ((diag, j + 1), (panel, 0)):
                for l in range(start, len(values)):
                    row = row_of(values[l], j) * inverse
                    values[l] = jnp.where(sub == j, row, values[l] - rest * row)
        for i in range(blocks):
            if i == k:
                continue
            for j in range(SUB):
                if k < blocks - 1:
                    left[i] = left[i] - cols[j][i] * row_of(panel[0], j)
                right[i] = right[i] - cols[j][i] * row_of(panel[1], j)
        left[k], right[k] = panel
    return right


def solve_kernel(*refs):
    *shares, mine_ref, theirs_ref = refs
    ne = (shares[0].shape[0] - SUB) // 2
    half = ne // 2
    count = ne // SUB

    def total(row):
        return functools.reduce(jnp.add, [s[row : row + SUB, :] for s in shares])

    lane = lax.broadcasted_iota(jnp.int32, (SUB, LANES), 1)
    sub = lax.broadcasted_iota(jnp.int32, (SUB, LANES), 0)
    damping = (ne - 1.0) + total(2 * ne) / ne
    left = []
    for i in range(count):
        x = total(i * SUB)
        left.append(jnp.where(lane % ne == SUB * i + sub, x + damping, x))
    right = eliminate(left, [total(ne + i * SUB) for i in range(count)])
    sorted_rows = [
        jnp.where(lane % ne < half, right[i], right[(i + count // 2) % count]) for i in range(count)
    ]
    turned = jnp.concatenate(sorted_rows, axis=0).T.astype(jnp.bfloat16)
    for r in range(2):
        mine_ref[r * half : (r + 1) * half, :] = turned[r * ne : r * ne + half]
        theirs_ref[r * half : (r + 1) * half, :] = turned[r * ne + half : (r + 1) * ne]


def anomaly_kernel(mine_ref, theirs_ref, out_ref):
    half = mine_ref.shape[0]
    mine = mine_ref[...].astype(jnp.float32)
    theirs = theirs_ref[...].astype(jnp.float32)
    total = jnp.sum(mine, axis=0, keepdims=True) + jnp.sum(theirs, axis=0, keepdims=True)
    center = total / (2 * half)
    out_ref[0:half, :] = (mine - center).astype(jnp.bfloat16)
    out_ref[half : 2 * half, :] = (theirs - center).astype(jnp.bfloat16)


def apply_kernel(mine_ref, theirs_ref, anomaly_ref, members_ref, regions_ref, out_ref, coeff_ref):
    half = members_ref.shape[0]
    rows = mine_ref.shape[0]
    coeff_ref[0:rows, :] = mine_ref[...]
    coeff_ref[rows : 2 * rows, :] = theirs_ref[...]
    core = lax.axis_index("mem")
    for b in range(members_ref.shape[1] // BLOCK):
        region = regions_ref[b]
        start = jnp.where(region // 2 == core, 0, rows) + (region % 2) * half
        coeff = coeff_ref[pl.ds(pl.multiple_of(start, half), half), :]
        span = slice(b * BLOCK, (b + 1) * BLOCK)
        delta = jnp.dot(coeff, anomaly_ref[:, span], preferred_element_type=jnp.float32)
        out_ref[:, span] = (members_ref[:, span].astype(jnp.float32) + delta).astype(jnp.bfloat16)


def exchanges(x, axis):
    size = lax.axis_size(axis)
    if size & (size - 1):
        return [lax.psum(x, axis)]
    parts, step = [x], 1
    while step < size:
        width = 4 if size // step >= 4 else 2
        x = functools.reduce(jnp.add, parts)
        parts = [x] + [
            lax.ppermute(x, axis, [(i, i ^ (m * step)) for i in range(size)]) for m in range(1, width)
        ]
        step *= width
    return parts


def body(members, observed, obs_error, obs_cells, perturbations, region_ids):
    half, cells = members.shape
    ne = 2 * half
    nobs = observed.shape[0]
    swap = [(0, 1), (1, 0)]
    other = lax.ppermute(members, "mem", swap)
    mine, onehot, predicted, innov, noise, rows = pl.pallas_call(
        prepare_kernel,
        out_shape=[
            pltpu.VMEM((half, cells), jnp.bfloat16),
            pltpu.VMEM((TILE, nobs), jnp.bfloat16),
            pltpu.VMEM((half, nobs), jnp.float32),
            pltpu.VMEM((half, nobs), jnp.bfloat16),
            pltpu.VMEM((half, nobs), jnp.bfloat16),
            pltpu.VMEM((SUB, nobs), jnp.float32),
        ],
        in_specs=[HBM] * 5 + [SMEM],
        out_specs=[VMEM] * 6,
        scratch_shapes=[
            pltpu.VMEM((1, nobs), jnp.int32),
            pltpu.VMEM((1, nobs), jnp.float32),
            pltpu.VMEM((1, nobs), jnp.float32),
            pltpu.VMEM((ne, nobs), jnp.bfloat16),
            pltpu.SemaphoreType.DMA((5,)),
        ],
        name="prepare",
    )(
        members,
        obs_cells.reshape(1, nobs),
        observed.reshape(1, nobs),
        obs_error.reshape(1, nobs),
        perturbations.T,
        region_ids,
    )
    sums = pl.pallas_call(
        stats_kernel,
        out_shape=pltpu.VMEM((2 * ne + SUB, 2 * ne), jnp.float32),
        in_specs=[VMEM] * 6,
        out_specs=VMEM,
        name="stats",
    )(*[near(x) for x in (other, onehot, predicted, innov, noise, rows)])
    anomaly = pl.pallas_call(
        anomaly_kernel,
        out_shape=pltpu.VMEM((ne, cells), jnp.bfloat16),
        in_specs=[VMEM] * 2,
        out_specs=VMEM,
        name="anomaly",
    )(near(mine), near(other))
    first, *others = exchanges(sums, "obs")
    others, anomaly = lax.optimization_barrier((others, anomaly))
    sums = functools.reduce(jnp.add, others, first)
    shares = exchanges(sums, "cells")
    coeff, theirs = pl.pallas_call(
        solve_kernel,
        out_shape=[pltpu.VMEM((ne, ne), jnp.bfloat16)] * 2,
        in_specs=[VMEM] * len(shares),
        out_specs=[VMEM] * 2,
        name="solve",
    )(*[near(s) for s in shares])
    theirs = lax.ppermute(theirs, "mem", swap)
    return pl.pallas_call(
        apply_kernel,
        out_shape=jax.ShapeDtypeStruct((half, cells), jnp.bfloat16),
        in_specs=[VMEM] * 4 + [SMEM],
        out_specs=VMEM,
        scratch_shapes=[pltpu.VMEM((2 * ne, ne), jnp.bfloat16)],
        name="apply",
    )(near(coeff), near(theirs), near(anomaly), near(mine), region_ids)


def solution(mesh):
    cut = ("groups", "cells", "obs")
    in_specs = (P("mem", cut), P(cut), P(cut), P(cut), P(cut, None), P(cut))
    return jax.shard_map(
        body, mesh=mesh, in_specs=in_specs, out_specs=P("mem", cut), check_vma=False
    )
```

```python
import functools

import jax
import jax.numpy as jnp
from jax import lax
from jax.experimental import pallas as pl
from jax.experimental.pallas import tpu as pltpu
from jax.sharding import PartitionSpec as P

NLOC = 4
BLOCK = 512
SUB = 8
LANES = 128
TILE = 256


VMEM = pl.BlockSpec(memory_space=pltpu.VMEM)
SMEM = pl.BlockSpec(memory_space=pltpu.SMEM)
HBM = pl.BlockSpec(memory_space=pl.ANY)


def near(x):
    return pltpu.with_memory_space_constraint(x, pltpu.VMEM)


def prepare_kernel(
    members_hbm, cells_hbm, observed_hbm, error_hbm, noise_hbm, regions_hbm,
    members_ref, onehot_ref, predicted_ref, innov_ref, noise_ref, rows_ref, cells_ref, observed_ref,
    error_ref, all_noise_ref, regions_ref, sems,
):
    moves = [
        pltpu.make_async_copy(src, dst, sems.at[i])
        for i, (src, dst) in enumerate(
            (
                (cells_hbm, cells_ref),
                (members_hbm, members_ref),
                (error_hbm, error_ref),
                (observed_hbm, observed_ref),
                (noise_hbm, all_noise_ref),
                (regions_hbm, regions_ref),
            )
        )
    ]
    for move in moves:
        move.start()
    half, cells = members_ref.shape
    nobs = cells_ref.shape[1]
    moves[0].wait()
    cell = cells_ref[...]
    part = cell // TILE
    onehot = lax.broadcasted_iota(jnp.int32, (TILE, nobs), 0) == cell - part * TILE
    onehot = onehot.astype(jnp.bfloat16)
    onehot_ref[...] = onehot
    moves[1].wait()
    predicted = predict(members_ref, onehot, part)
    predicted_ref[...] = predicted
    moves[2].wait()
    moves[3].wait()
    inverse = 1.0 / error_ref[...]
    moves[4].wait()
    core = lax.axis_index("mem")
    noise = all_noise_ref[pl.ds(pl.multiple_of(core * half, half), half), :].astype(jnp.float32)
    innov = (observed_ref[...] - predicted) * inverse + noise
    innov_ref[...] = innov.astype(jnp.bfloat16)
    noise_ref[...] = all_noise_ref[pl.ds(pl.multiple_of((1 - core) * half, half), half), :]
    moves[5].wait()
    block = cell // BLOCK
    region = jnp.zeros_like(cell)
    for b in range(cells // BLOCK):
        region = jnp.where(block == b, regions_ref[b], region)
    rows_ref[0:1, :] = observed_ref[...]
    rows_ref[1:2, :] = inverse
    rows_ref[2:3, :] = part.astype(jnp.float32)
    rows_ref[3:4, :] = region.astype(jnp.float32)
    rows_ref[4:5, :] = jnp.sum(predicted, axis=0, keepdims=True)
    rows_ref[5:6, :] = jnp.sum(innov * innov, axis=0, keepdims=True)
    rows_ref[6:8, :] = jnp.zeros((2, nobs), jnp.float32)


def predict(members_ref, onehot, part):
    members, cells = members_ref.shape
    values = jnp.zeros((members, part.shape[1]), jnp.float32)
    for p in range(cells // TILE):
        picked = jnp.dot(
            members_ref[:, p * TILE : (p + 1) * TILE], onehot, preferred_element_type=jnp.float32
        )
        values = jnp.where(part == p, picked, values)
    return values + 0.2 * values * values * values


def stats_kernel(
    theirs_ref, onehot_ref, predicted_ref, innov_ref, noise_ref, rows_ref,
    sums_ref, sent_ref, half_ref, sens_ref, innovs_ref,
):
    half = theirs_ref.shape[0]
    ne = 2 * half
    pairs = NLOC // 2
    core = lax.axis_index("mem")
    at_mine = pl.ds(pl.multiple_of(core * half, half), half)
    at_theirs = pl.ds(pl.multiple_of((1 - core) * half, half), half)
    observed, inverse, part, region, mine_sum, mine_square = [rows_ref[i : i + 1, :] for i in range(6)]
    mine = predicted_ref[...]
    theirs = predict(theirs_ref, onehot_ref[...], part)
    innov = (observed - theirs) * inverse + noise_ref[...].astype(jnp.float32)
    square = mine_square + jnp.sum(innov * innov, axis=0, keepdims=True)
    pmean = (mine_sum + jnp.sum(theirs, axis=0, keepdims=True)) / ne
    sens_ref[at_mine, :] = ((mine - pmean) * inverse).astype(jnp.bfloat16)
    sens_ref[at_theirs, :] = ((theirs - pmean) * inverse).astype(jnp.bfloat16)
    innovs_ref[at_mine, :] = innov_ref[...]
    innovs_ref[at_theirs, :] = innov.astype(jnp.bfloat16)
    sens = sens_ref[...]
    inside = [region == r for r in range(NLOC)]
    lane = lax.broadcasted_iota(jnp.int32, (SUB, LANES), 1)
    on_diagonal = lax.broadcasted_iota(jnp.int32, (ne, LANES), 1) % ne == lax.broadcasted_iota(
        jnp.int32, (ne, LANES), 0
    )

    def product(x):
        masked = jnp.concatenate([jnp.where(m, x, jnp.zeros_like(x)) for m in inside], axis=0)
        return lax.dot_general(
            sens, masked, (((1,), (1,)), ((), ())), preferred_element_type=jnp.float32
        )

    gram = product(sens)
    cross = product(innovs_ref[...])
    misfits = [
        jnp.sum(jnp.where(m, square, jnp.float32(0.0)), axis=1, keepdims=True) for m in inside
    ]
    for p in range(pairs):
        lanes = slice(p * LANES, (p + 1) * LANES)
        g = gram[:, lanes]
        row = 2 * p * ne
        sums_ref[row : row + ne, :] = jnp.where(on_diagonal, 0.0, g)
        sums_ref[row + ne : row + 2 * ne, :] = cross[:, lanes] + g
        tail = 2 * pairs * ne
        sums_ref[tail + p : tail + p + 1, :] = jnp.where(
            lane < ne, misfits[2 * p], misfits[2 * p + 1]
        )[0:1]
        sums_ref[tail + pairs + p : tail + pairs + p + 1, :] = jnp.sum(
            jnp.where(on_diagonal, g, 0.0), axis=0, keepdims=True
        )
    pack(sums_ref, sent_ref, half_ref)


def pack(sums_ref, sent_ref, half_ref):
    rows = sums_ref.shape[0] - NLOC
    sent_ref[0:rows, :] = sums_ref[0:rows, :].astype(jnp.bfloat16)
    left = sums_ref[rows : rows + NLOC, :]
    parts = []
    for _ in range(3):
        part = left.astype(jnp.bfloat16).astype(jnp.float32)
        parts.append(part)
        left = left - part
    parts.append(jnp.zeros_like(left))
    tail = jnp.concatenate(parts, axis=0).astype(jnp.bfloat16)
    sent_ref[rows : rows + 4 * NLOC, :] = tail
    half = rows // 2
    start = pl.multiple_of(lax.axis_index("mem") * half, half)
    half_ref[0:half, :] = sums_ref[pl.ds(start, half), :].astype(jnp.bfloat16)
    half_ref[half : half + 4 * NLOC, :] = tail


def fold_kernel(*refs):
    sums_ref, shared_ref, *got, out_ref = refs
    rows = sums_ref.shape[0] - NLOC
    half = rows // 2
    core = lax.axis_index("mem")
    if got:
        out_ref[0:rows, :] = functools.reduce(
            jnp.add, [g[0:rows, :].astype(jnp.float32) for g in got]
        )
    else:
        out_ref[...] = jnp.zeros_like(out_ref)
    mine = pl.ds(pl.multiple_of(core * half, half), half)
    out_ref[mine, :] += sums_ref[mine, :] + shared_ref[0:half, :].astype(jnp.float32)
    tails = [whole(g[rows : rows + 4 * NLOC, :]) for g in got]
    both = sums_ref[rows : rows + NLOC, :] + whole(shared_ref[half : half + 4 * NLOC, :])
    out_ref[rows : rows + NLOC, :] = functools.reduce(
        jnp.add, tails, jnp.where(core == 0, both, jnp.zeros_like(both))
    )


def whole(parts):
    parts = parts.astype(jnp.float32)
    return parts[0:NLOC] + parts[NLOC : 2 * NLOC] + parts[2 * NLOC : 3 * NLOC]


def repack_kernel(mine_ref, theirs_ref, sums_ref, sent_ref, half_ref):
    sums_ref[...] = mine_ref[...] + theirs_ref[...]
    pack(sums_ref, sent_ref, half_ref)


def row_of(x, j):
    return jnp.broadcast_to(x[j : j + 1, :], x.shape)


def lane_of(x, c, lane):
    half = LANES // 2
    index = jnp.where(lane < half, c, half + c)
    return jnp.take_along_axis(x, index, axis=1, mode="promise_in_bounds")


def eliminate(systems):
    blocks = len(systems[0][0])
    sub = lax.broadcasted_iota(jnp.int32, (SUB, LANES), 0)
    lane = lax.broadcasted_iota(jnp.int32, (SUB, LANES), 1)
    for k in range(blocks):
        cols = [
            [[lane_of(left[i], SUB * k + j, lane) for i in range(blocks)] for j in range(SUB)]
            for left, _ in systems
        ]
        diags = [[col[j][k] for j in range(SUB)] for col in cols]
        panels = [[left[k], right[k]] for left, right in systems]
        for j in range(SUB):
            for diag, panel in zip(diags, panels):
                inverse = 1.0 / row_of(diag[j], j)
                rest = jnp.where(sub == j, 0.0, diag[j])
                for values, start in ((diag, j + 1), (panel, 0)):
                    for l in range(start, len(values)):
                        row = row_of(values[l], j) * inverse
                        values[l] = jnp.where(sub == j, row, values[l] - rest * row)
        for (left, right), panel, col in zip(systems, panels, cols):
            for i in range(blocks):
                if i == k:
                    continue
                for j in range(SUB):
                    if k < blocks - 1:
                        left[i] = left[i] - col[j][i] * row_of(panel[0], j)
                    right[i] = right[i] - col[j][i] * row_of(panel[1], j)
            left[k], right[k] = panel


def finish_kernel(
    mine_ref, theirs_ref, anomaly_ref, members_ref, regions_hbm, out_hbm,
    coeff_ref, regions_ref, updated_ref, sems,
):
    half, cells = members_ref.shape
    ne = 2 * half
    count = ne // SUB
    pairs = NLOC // 2
    load = pltpu.make_async_copy(regions_hbm, regions_ref, sems.at[0])
    load.start()

    def total(row, rows=SUB):
        return mine_ref[row : row + rows, :] + theirs_ref[row : row + rows, :]

    lane = lax.broadcasted_iota(jnp.int32, (SUB, LANES), 1)
    sub = lax.broadcasted_iota(jnp.int32, (SUB, LANES), 0)
    tail = total(2 * pairs * ne, NLOC)
    systems = []
    for p in range(pairs):
        diagonal = jnp.broadcast_to(tail[pairs + p : pairs + p + 1], (SUB, LANES))
        damped = diagonal + ((ne - 1.0) + jnp.broadcast_to(tail[p : p + 1], (SUB, LANES)) / ne)
        left, right = [], []
        for i in range(count):
            gram = total(2 * p * ne + i * SUB)
            here = lane % ne == SUB * i + sub
            left.append(jnp.where(here, damped, gram))
            right.append(total((2 * p + 1) * ne + i * SUB) - jnp.where(here, diagonal, gram))
        systems.append((left, right))
    eliminate(systems)
    for p, (_, right) in enumerate(systems):
        turned = jnp.concatenate(right, axis=0).T
        coeff_ref[2 * p * ne : 2 * (p + 1) * ne, :] = turned.astype(jnp.bfloat16)
    core = lax.axis_index("mem")
    load.wait()
    stores = []
    for b in range(cells // BLOCK):
        start = pl.multiple_of(regions_ref[b] * ne + core * half, half)
        span = slice(b * BLOCK, (b + 1) * BLOCK)
        delta = jnp.dot(
            coeff_ref[pl.ds(start, half), :], anomaly_ref[:, span], preferred_element_type=jnp.float32
        )
        updated_ref[:, span] = (members_ref[:, span].astype(jnp.float32) + delta).astype(jnp.bfloat16)
        stores.append(
            pltpu.make_async_copy(updated_ref.at[:, span], out_hbm.at[:, span], sems.at[1 + b])
        )
        stores[-1].start()
    for store in stores:
        store.wait()


def anomaly_kernel(mine_ref, theirs_ref, out_ref):
    half = mine_ref.shape[0]
    core = lax.axis_index("mem")
    mine = mine_ref[...].astype(jnp.float32)
    theirs = theirs_ref[...].astype(jnp.float32)
    total = jnp.sum(mine, axis=0, keepdims=True) + jnp.sum(theirs, axis=0, keepdims=True)
    center = total / (2 * half)
    at_mine = pl.ds(pl.multiple_of(core * half, half), half)
    at_theirs = pl.ds(pl.multiple_of((1 - core) * half, half), half)
    out_ref[at_mine, :] = (mine - center).astype(jnp.bfloat16)
    out_ref[at_theirs, :] = (theirs - center).astype(jnp.bfloat16)


def stages(sizes):
    bits = [
        [(axis, 1 << i) for i in range(size.bit_length() - 1)] for axis, size in enumerate(sizes)
    ]
    first, last = bits
    groups = []
    while first or last:
        group = first[:2] + last[:1]
        first, last = first[2:], last[1:]
        groups.append(group)
    return groups


PARTNERS = {1: ((), (), 1), 2: ((1,), (3,), 2), 3: ((4, 5, 3), (1, 6, 7), 2)}


def partners(group, sizes):
    low, high, shared = PARTNERS[len(group)]

    def step(mask):
        way = [0, 0]
        for i, (axis, bit) in enumerate(group):
            if mask >> i & 1:
                way[axis] |= bit
        return way

    def place(c, o, m):
        return (c * sizes[1] + o) * 2 + m

    ways = [(step(a), step(b)) for a, b in zip(low, high)] + [(step(shared), step(shared))]
    return [
        [
            (place(c, o, m), place(c ^ way[m][0], o ^ way[m][1], m))
            for c in range(sizes[0])
            for o in range(sizes[1])
            for m in range(2)
        ]
        for way in ways
    ]


def body(members, observed, obs_error, obs_cells, perturbations, region_ids):
    half, cells = members.shape
    ne = 2 * half
    nobs = observed.shape[0]
    blocks = region_ids.shape[0]
    rows = NLOC * ne
    swap = [(0, 1), (1, 0)]
    other = lax.ppermute(members, "mem", swap)
    mine, onehot, predicted, innov, noise, lines = pl.pallas_call(
        prepare_kernel,
        out_shape=[
            pltpu.VMEM((half, cells), jnp.bfloat16),
            pltpu.VMEM((TILE, nobs), jnp.bfloat16),
            pltpu.VMEM((half, nobs), jnp.float32),
            pltpu.VMEM((half, nobs), jnp.bfloat16),
            pltpu.VMEM((half, nobs), jnp.bfloat16),
            pltpu.VMEM((SUB, nobs), jnp.float32),
        ],
        in_specs=[HBM] * 6,
        out_specs=[VMEM] * 6,
        scratch_shapes=[
            pltpu.VMEM((1, nobs), jnp.int32),
            pltpu.VMEM((1, nobs), jnp.float32),
            pltpu.VMEM((1, nobs), jnp.float32),
            pltpu.VMEM((ne, nobs), jnp.bfloat16),
            pltpu.SMEM((blocks,), jnp.int32),
            pltpu.SemaphoreType.DMA((6,)),
        ],
        name="prepare",
    )(
        members,
        obs_cells.reshape(1, nobs),
        observed.reshape(1, nobs),
        obs_error.reshape(1, nobs),
        perturbations.T,
        region_ids,
    )
    sums_shape = pltpu.VMEM((rows + NLOC, LANES), jnp.float32)
    packed = [
        sums_shape,
        pltpu.VMEM((rows + 4 * NLOC, LANES), jnp.bfloat16),
        pltpu.VMEM((rows // 2 + 4 * NLOC, LANES), jnp.bfloat16),
    ]
    sums, sent, shared = pl.pallas_call(
        stats_kernel,
        out_shape=packed,
        in_specs=[VMEM] * 6,
        out_specs=[VMEM] * 3,
        scratch_shapes=[pltpu.VMEM((ne, nobs), jnp.bfloat16)] * 2,
        name="stats",
    )(*[near(x) for x in (other, onehot, predicted, innov, noise, lines)])
    anomaly = pl.pallas_call(
        anomaly_kernel,
        out_shape=pltpu.VMEM((ne, cells), jnp.bfloat16),
        in_specs=[VMEM] * 2,
        out_specs=VMEM,
        name="anomaly",
    )(near(mine), near(other))
    axes = ("cells", "obs", "mem")
    sizes = (lax.axis_size("cells"), lax.axis_size("obs"))
    groups = stages(sizes)
    for number, group in enumerate(groups):
        *single, common = partners(group, sizes)
        got = [lax.ppermute(sent, axes, p) for p in single]
        got.insert(0, lax.ppermute(shared, axes, common))
        if number == 0:
            got, anomaly = lax.optimization_barrier((got, anomaly))
        total = pl.pallas_call(
            fold_kernel,
            out_shape=sums_shape,
            in_specs=[VMEM] * (1 + len(got)),
            out_specs=VMEM,
            name="fold",
        )(near(sums), *[near(g) for g in got])
        theirs = lax.ppermute(total, "mem", swap)
        if number < len(groups) - 1:
            sums, sent, shared = pl.pallas_call(
                repack_kernel,
                out_shape=packed,
                in_specs=[VMEM] * 2,
                out_specs=[VMEM] * 3,
                name="repack",
            )(near(total), near(theirs))
    return pl.pallas_call(
        finish_kernel,
        out_shape=jax.ShapeDtypeStruct((half, cells), jnp.bfloat16),
        in_specs=[VMEM] * 4 + [HBM],
        out_specs=HBM,
        scratch_shapes=[
            pltpu.VMEM((rows, ne), jnp.bfloat16),
            pltpu.SMEM((blocks,), jnp.int32),
            pltpu.VMEM((half, cells), jnp.bfloat16),
            pltpu.SemaphoreType.DMA((1 + blocks,)),
        ],
        name="finish",
    )(near(total), near(theirs), near(anomaly), near(mine), region_ids)


def solution(mesh):
    cut = ("groups", "cells", "obs")
    in_specs = (P("mem", cut), P(cut), P(cut), P(cut), P(cut, None), P(cut))
    return jax.shard_map(
        body, mesh=mesh, in_specs=in_specs, out_specs=P("mem", cut), check_vma=False
    )
```

```python
import functools

import jax
import jax.numpy as jnp
from jax import lax
from jax.experimental import pallas as pl
from jax.experimental.pallas import tpu as pltpu
from jax.sharding import PartitionSpec as P

NLOC = 4
BLOCK = 512
SUB = 8
LANES = 128
TILE = 256


VMEM = pl.BlockSpec(memory_space=pltpu.VMEM)
SMEM = pl.BlockSpec(memory_space=pltpu.SMEM)
HBM = pl.BlockSpec(memory_space=pl.ANY)


def near(x):
    return pltpu.with_memory_space_constraint(x, pltpu.VMEM)


def prepare_kernel(
    members_hbm, cells_hbm, observed_hbm, error_hbm, noise_hbm, regions_hbm,
    members_ref, onehot_ref, predicted_ref, innov_ref, noise_ref, rows_ref, cells_ref, observed_ref,
    error_ref, all_noise_ref, regions_ref, sems,
):
    moves = [
        pltpu.make_async_copy(src, dst, sems.at[i])
        for i, (src, dst) in enumerate(
            (
                (cells_hbm, cells_ref),
                (members_hbm, members_ref),
                (error_hbm, error_ref),
                (observed_hbm, observed_ref),
                (noise_hbm, all_noise_ref),
                (regions_hbm, regions_ref),
            )
        )
    ]
    for move in moves:
        move.start()
    half, cells = members_ref.shape
    nobs = cells_ref.shape[1]
    moves[0].wait()
    cell = cells_ref[...]
    part = cell // TILE
    onehot = lax.broadcasted_iota(jnp.int32, (TILE, nobs), 0) == cell - part * TILE
    onehot = onehot.astype(jnp.bfloat16)
    onehot_ref[...] = onehot
    moves[1].wait()
    predicted = predict(members_ref, onehot, part)
    predicted_ref[...] = predicted
    moves[2].wait()
    moves[3].wait()
    inverse = 1.0 / error_ref[...]
    moves[4].wait()
    core = lax.axis_index("mem")
    noise = all_noise_ref[pl.ds(pl.multiple_of(core * half, half), half), :].astype(jnp.float32)
    innov = (observed_ref[...] - predicted) * inverse + noise
    innov_ref[...] = innov.astype(jnp.bfloat16)
    noise_ref[...] = all_noise_ref[pl.ds(pl.multiple_of((1 - core) * half, half), half), :]
    moves[5].wait()
    block = cell // BLOCK
    region = jnp.zeros_like(cell)
    for b in range(cells // BLOCK):
        region = jnp.where(block == b, regions_ref[b], region)
    rows_ref[0:1, :] = observed_ref[...]
    rows_ref[1:2, :] = inverse
    rows_ref[2:3, :] = part.astype(jnp.float32)
    rows_ref[3:4, :] = region.astype(jnp.float32)
    rows_ref[4:5, :] = jnp.sum(predicted, axis=0, keepdims=True)
    rows_ref[5:6, :] = jnp.sum(innov * innov, axis=0, keepdims=True)
    rows_ref[6:8, :] = jnp.zeros((2, nobs), jnp.float32)


def predict(members_ref, onehot, part):
    members, cells = members_ref.shape
    tiles = cells // TILE
    stacked = jnp.concatenate(
        [members_ref[:, p * TILE : (p + 1) * TILE] for p in range(tiles)], axis=0
    )
    picked = jnp.dot(stacked, onehot, preferred_element_type=jnp.float32)
    values = picked[0:members]
    for p in range(1, tiles):
        values = jnp.where(part == p, picked[p * members : (p + 1) * members], values)
    return values + 0.2 * values * values * values


def stats_kernel(
    theirs_ref, onehot_ref, predicted_ref, innov_ref, noise_ref, rows_ref,
    sums_ref, sent_ref, half_ref, sens_ref, innovs_ref,
):
    half = theirs_ref.shape[0]
    ne = 2 * half
    pairs = NLOC // 2
    core = lax.axis_index("mem")
    at_mine = pl.ds(pl.multiple_of(core * half, half), half)
    at_theirs = pl.ds(pl.multiple_of((1 - core) * half, half), half)
    observed, inverse, part, region, mine_sum, mine_square = [rows_ref[i : i + 1, :] for i in range(6)]
    mine = predicted_ref[...]
    theirs = predict(theirs_ref, onehot_ref[...], part)
    innov = (observed - theirs) * inverse + noise_ref[...].astype(jnp.float32)
    square = mine_square + jnp.sum(innov * innov, axis=0, keepdims=True)
    pmean = (mine_sum + jnp.sum(theirs, axis=0, keepdims=True)) / ne
    sens_ref[at_mine, :] = ((mine - pmean) * inverse).astype(jnp.bfloat16)
    sens_ref[at_theirs, :] = ((theirs - pmean) * inverse).astype(jnp.bfloat16)
    innovs_ref[at_mine, :] = innov_ref[...]
    innovs_ref[at_theirs, :] = innov.astype(jnp.bfloat16)
    sens = sens_ref[...]
    inside = [region == r for r in range(NLOC)]
    lane = lax.broadcasted_iota(jnp.int32, (SUB, LANES), 1)
    column = lax.broadcasted_iota(jnp.int32, (ne, LANES), 1) % ne
    below = column < lax.broadcasted_iota(jnp.int32, (ne, LANES), 0)
    on_diagonal = column == lax.broadcasted_iota(jnp.int32, (ne, LANES), 0)

    def product(x):
        masked = jnp.concatenate([jnp.where(m, x, jnp.zeros_like(x)) for m in inside], axis=0)
        return lax.dot_general(
            sens, masked, (((1,), (1,)), ((), ())), preferred_element_type=jnp.float32
        )

    gram = product(sens)
    cross = product(innovs_ref[...])
    misfits = [
        jnp.sum(jnp.where(m, square, jnp.float32(0.0)), axis=1, keepdims=True) for m in inside
    ]
    for p in range(pairs):
        lanes = slice(p * LANES, (p + 1) * LANES)
        g = gram[:, lanes]
        row = (1 + p) * ne
        sums_ref[row : row + ne, :] = cross[:, lanes] + g
        tail = (1 + pairs) * ne
        sums_ref[tail + p : tail + p + 1, :] = jnp.where(
            lane < ne, misfits[2 * p], misfits[2 * p + 1]
        )[0:1]
        sums_ref[tail + pairs + p : tail + pairs + p + 1, :] = jnp.sum(
            jnp.where(on_diagonal, g, 0.0), axis=0, keepdims=True
        )
    sums_ref[0:ne, :] = jnp.where(
        on_diagonal, 0.0, jnp.where(below, gram[:, 0:LANES], gram[:, LANES : 2 * LANES])
    )
    pack(sums_ref, sent_ref, half_ref)


def pack(sums_ref, sent_ref, half_ref):
    rows = sums_ref.shape[0] - NLOC
    sent_ref[0:rows, :] = sums_ref[0:rows, :].astype(jnp.bfloat16)
    left = sums_ref[rows : rows + NLOC, :]
    parts = []
    for _ in range(3):
        part = left.astype(jnp.bfloat16).astype(jnp.float32)
        parts.append(part)
        left = left - part
    parts.append(jnp.zeros_like(left))
    tail = jnp.concatenate(parts, axis=0).astype(jnp.bfloat16)
    sent_ref[rows : rows + 4 * NLOC, :] = tail
    half = rows // 2
    start = pl.multiple_of(lax.axis_index("mem") * half, half)
    half_ref[0:half, :] = sums_ref[pl.ds(start, half), :].astype(jnp.bfloat16)
    half_ref[half : half + 4 * NLOC, :] = tail


def fold_kernel(*refs):
    sums_ref, shared_ref, *got, out_ref = refs
    rows = sums_ref.shape[0] - NLOC
    half = rows // 2
    core = lax.axis_index("mem")
    if got:
        out_ref[0:rows, :] = functools.reduce(
            jnp.add, [g[0:rows, :].astype(jnp.float32) for g in got]
        )
    else:
        out_ref[...] = jnp.zeros_like(out_ref)
    mine = pl.ds(pl.multiple_of(core * half, half), half)
    out_ref[mine, :] += sums_ref[mine, :] + shared_ref[0:half, :].astype(jnp.float32)
    tails = [whole(g[rows : rows + 4 * NLOC, :]) for g in got]
    both = sums_ref[rows : rows + NLOC, :] + whole(shared_ref[half : half + 4 * NLOC, :])
    out_ref[rows : rows + NLOC, :] = functools.reduce(
        jnp.add, tails, jnp.where(core == 0, both, jnp.zeros_like(both))
    )


def whole(parts):
    parts = parts.astype(jnp.float32)
    return parts[0:NLOC] + parts[NLOC : 2 * NLOC] + parts[2 * NLOC : 3 * NLOC]


def repack_kernel(mine_ref, theirs_ref, sums_ref, sent_ref, half_ref):
    sums_ref[...] = mine_ref[...] + theirs_ref[...]
    pack(sums_ref, sent_ref, half_ref)


def row_of(x, j):
    return jnp.broadcast_to(x[j : j + 1, :], x.shape)


def lane_of(x, c, lane):
    half = LANES // 2
    index = jnp.where(lane < half, c, half + c)
    return jnp.take_along_axis(x, index, axis=1, mode="promise_in_bounds")


def eliminate(systems, blocks):
    sub = lax.broadcasted_iota(jnp.int32, (SUB, LANES), 0)
    lane = lax.broadcasted_iota(jnp.int32, (SUB, LANES), 1)
    for k in blocks:
        cols = [
            [{i: lane_of(left[i], SUB * k + j, lane) for i in blocks} for j in range(SUB)]
            for left, _ in systems
        ]
        diags = [[col[j][k] for j in range(SUB)] for col in cols]
        panels = [[left[k], right[k]] for left, right in systems]
        scales = [None] * len(systems)
        for j in range(SUB):
            for s, (diag, panel) in enumerate(zip(diags, panels)):
                inverse = 1.0 / row_of(diag[j], j)
                factor = jnp.where(sub == j, 0.0, diag[j]) * inverse
                scales[s] = inverse if j == 0 else jnp.where(sub == j, inverse, scales[s])
                for values, start in ((diag, j + 1), (panel, 0)):
                    for l in range(start, len(values)):
                        values[l] = values[l] - factor * row_of(values[l], j)
        panels = [[x * scale for x in panel] for panel, scale in zip(panels, scales)]
        for (left, right), panel, col in zip(systems, panels, cols):
            for i in blocks:
                if i == k:
                    continue
                for j in range(SUB):
                    left[i] = left[i] - col[j][i] * row_of(panel[0], j)
                    right[i] = right[i] - col[j][i] * row_of(panel[1], j)
            left[k], right[k] = panel


def times(rows, below, above, values):
    count = len(values)
    lane = lax.broadcasted_iota(jnp.int32, (SUB, LANES * len(values[0])), 1) % LANES
    zero = [jnp.zeros(lane.shape, jnp.float32)]
    stacked = [jnp.concatenate(v, axis=1) for v in values]
    matrix = []
    for region in range(2):
        kept = [
            jnp.where((lane < LANES // 2) if region == 0 else (lane >= LANES // 2), v, 0.0) for v in stacked
        ]
        matrix += zero * below + kept + zero * above
    product = jnp.dot(
        jnp.concatenate(rows, axis=0),
        jnp.concatenate(matrix, axis=0),
        precision=lax.Precision.HIGHEST,
        preferred_element_type=jnp.float32,
    )
    return [product[i * SUB : (i + 1) * SUB] for i in range(count)]


def solve(systems):
    count = len(systems[0][0])
    top, bottom = range(count // 2), range(count // 2, count)
    eliminate(systems, top)
    for left, right in systems:
        product = times(
            [left[i] for i in bottom], 0, count // 2, [(left[i], right[i]) for i in top]
        )
        for i, p in zip(bottom, product):
            left[i] = left[i] - p[:, 0:LANES]
            right[i] = right[i] - p[:, LANES:]
    eliminate(systems, bottom)
    for left, right in systems:
        product = times([left[i] for i in top], count // 2, 0, [(right[i],) for i in bottom])
        for i, p in zip(top, product):
            right[i] = right[i] - p


def finish_kernel(
    mine_ref, theirs_ref, anomaly_ref, members_ref, regions_hbm, out_hbm,
    coeff_ref, regions_ref, updated_ref, sems,
):
    half, cells = members_ref.shape
    ne = 2 * half
    count = ne // SUB
    pairs = NLOC // 2
    load = pltpu.make_async_copy(regions_hbm, regions_ref, sems.at[0])
    load.start()

    def total(row, rows=SUB):
        return mine_ref[row : row + rows, :] + theirs_ref[row : row + rows, :]

    lane = lax.broadcasted_iota(jnp.int32, (SUB, LANES), 1)
    sub = lax.broadcasted_iota(jnp.int32, (SUB, LANES), 0)
    tail = total((1 + pairs) * ne, NLOC)
    triangles = total(0, ne)
    turned = triangles.T
    turned = jnp.concatenate([turned[0:ne], turned[ne : 2 * ne]], axis=1)
    systems = []
    for p in range(pairs):
        diagonal = jnp.broadcast_to(tail[pairs + p : pairs + p + 1], (SUB, LANES))
        damped = diagonal + ((ne - 1.0) + jnp.broadcast_to(tail[p : p + 1], (SUB, LANES)) / ne)
        left, right = [], []
        for i in range(count):
            given = (lane % ne < SUB * i + sub) if p == 0 else (lane % ne > SUB * i + sub)
            here = lane % ne == SUB * i + sub
            block = slice(i * SUB, (i + 1) * SUB)
            gram = jnp.where(given, triangles[block], turned[block])
            left.append(jnp.where(here, damped, gram))
            right.append(total((1 + p) * ne + i * SUB) - jnp.where(here, diagonal, gram))
        systems.append((left, right))
    solve(systems)
    for p, (_, right) in enumerate(systems):
        turned = jnp.concatenate(right, axis=0).T
        coeff_ref[2 * p * ne : 2 * (p + 1) * ne, :] = turned.astype(jnp.bfloat16)
    core = lax.axis_index("mem")
    load.wait()
    stores = []
    for b in range(cells // BLOCK):
        start = pl.multiple_of(regions_ref[b] * ne + core * half, half)
        span = slice(b * BLOCK, (b + 1) * BLOCK)
        delta = jnp.dot(
            coeff_ref[pl.ds(start, half), :], anomaly_ref[:, span], preferred_element_type=jnp.float32
        )
        updated_ref[:, span] = (members_ref[:, span].astype(jnp.float32) + delta).astype(jnp.bfloat16)
        stores.append(
            pltpu.make_async_copy(updated_ref.at[:, span], out_hbm.at[:, span], sems.at[1 + b])
        )
        stores[-1].start()
    for store in stores:
        store.wait()


def anomaly_kernel(mine_ref, theirs_ref, out_ref):
    half = mine_ref.shape[0]
    core = lax.axis_index("mem")
    mine = mine_ref[...].astype(jnp.float32)
    theirs = theirs_ref[...].astype(jnp.float32)
    total = jnp.sum(mine, axis=0, keepdims=True) + jnp.sum(theirs, axis=0, keepdims=True)
    center = total / (2 * half)
    at_mine = pl.ds(pl.multiple_of(core * half, half), half)
    at_theirs = pl.ds(pl.multiple_of((1 - core) * half, half), half)
    out_ref[at_mine, :] = (mine - center).astype(jnp.bfloat16)
    out_ref[at_theirs, :] = (theirs - center).astype(jnp.bfloat16)


def stages(sizes):
    bits = [
        [(axis, 1 << i) for i in range(size.bit_length() - 1)] for axis, size in enumerate(sizes)
    ]
    first, last = bits
    groups = []
    while first or last:
        group = first[:2] + last[:1]
        first, last = first[2:], last[1:]
        groups.append(group)
    return groups


PARTNERS = {1: ((), (), 1), 2: ((1,), (3,), 2), 3: ((4, 5, 3), (1, 6, 7), 2)}


def partners(group, sizes):
    low, high, shared = PARTNERS[len(group)]

    def step(mask):
        way = [0, 0]
        for i, (axis, bit) in enumerate(group):
            if mask >> i & 1:
                way[axis] |= bit
        return way

    def place(c, o, m):
        return (c * sizes[1] + o) * 2 + m

    ways = [(step(a), step(b)) for a, b in zip(low, high)] + [(step(shared), step(shared))]
    return [
        [
            (place(c, o, m), place(c ^ way[m][0], o ^ way[m][1], m))
            for c in range(sizes[0])
            for o in range(sizes[1])
            for m in range(2)
        ]
        for way in ways
    ]


def body(members, observed, obs_error, obs_cells, perturbations, region_ids):
    half, cells = members.shape
    ne = 2 * half
    nobs = observed.shape[0]
    blocks = region_ids.shape[0]
    rows = (1 + NLOC // 2) * ne
    swap = [(0, 1), (1, 0)]
    other = lax.ppermute(members, "mem", swap)
    mine, onehot, predicted, innov, noise, lines = pl.pallas_call(
        prepare_kernel,
        out_shape=[
            pltpu.VMEM((half, cells), jnp.bfloat16),
            pltpu.VMEM((TILE, nobs), jnp.bfloat16),
            pltpu.VMEM((half, nobs), jnp.float32),
            pltpu.VMEM((half, nobs), jnp.bfloat16),
            pltpu.VMEM((half, nobs), jnp.bfloat16),
            pltpu.VMEM((SUB, nobs), jnp.float32),
        ],
        in_specs=[HBM] * 6,
        out_specs=[VMEM] * 6,
        scratch_shapes=[
            pltpu.VMEM((1, nobs), jnp.int32),
            pltpu.VMEM((1, nobs), jnp.float32),
            pltpu.VMEM((1, nobs), jnp.float32),
            pltpu.VMEM((ne, nobs), jnp.bfloat16),
            pltpu.SMEM((blocks,), jnp.int32),
            pltpu.SemaphoreType.DMA((6,)),
        ],
        name="prepare",
    )(
        members,
        obs_cells.reshape(1, nobs),
        observed.reshape(1, nobs),
        obs_error.reshape(1, nobs),
        perturbations.T,
        region_ids,
    )
    sums_shape = pltpu.VMEM((rows + NLOC, LANES), jnp.float32)
    packed = [
        sums_shape,
        pltpu.VMEM((rows + 4 * NLOC, LANES), jnp.bfloat16),
        pltpu.VMEM((rows // 2 + 4 * NLOC, LANES), jnp.bfloat16),
    ]
    sums, sent, shared = pl.pallas_call(
        stats_kernel,
        out_shape=packed,
        in_specs=[VMEM] * 6,
        out_specs=[VMEM] * 3,
        scratch_shapes=[pltpu.VMEM((ne, nobs), jnp.bfloat16)] * 2,
        name="stats",
    )(*[near(x) for x in (other, onehot, predicted, innov, noise, lines)])
    anomaly = pl.pallas_call(
        anomaly_kernel,
        out_shape=pltpu.VMEM((ne, cells), jnp.bfloat16),
        in_specs=[VMEM] * 2,
        out_specs=VMEM,
        name="anomaly",
    )(near(mine), near(other))
    axes = ("cells", "obs", "mem")
    sizes = (lax.axis_size("cells"), lax.axis_size("obs"))
    groups = stages(sizes)
    for number, group in enumerate(groups):
        *single, common = partners(group, sizes)
        got = [lax.ppermute(sent, axes, p) for p in single]
        got.insert(0, lax.ppermute(shared, axes, common))
        if number == 0:
            got, anomaly = lax.optimization_barrier((got, anomaly))
        total = pl.pallas_call(
            fold_kernel,
            out_shape=sums_shape,
            in_specs=[VMEM] * (1 + len(got)),
            out_specs=VMEM,
            name="fold",
        )(near(sums), *[near(g) for g in got])
        theirs = lax.ppermute(total, "mem", swap)
        if number < len(groups) - 1:
            sums, sent, shared = pl.pallas_call(
                repack_kernel,
                out_shape=packed,
                in_specs=[VMEM] * 2,
                out_specs=[VMEM] * 3,
                name="repack",
            )(near(total), near(theirs))
    return pl.pallas_call(
        finish_kernel,
        out_shape=jax.ShapeDtypeStruct((half, cells), jnp.bfloat16),
        in_specs=[VMEM] * 4 + [HBM],
        out_specs=HBM,
        scratch_shapes=[
            pltpu.VMEM((NLOC * ne, ne), jnp.bfloat16),
            pltpu.SMEM((blocks,), jnp.int32),
            pltpu.VMEM((half, cells), jnp.bfloat16),
            pltpu.SemaphoreType.DMA((1 + blocks,)),
        ],
        name="finish",
    )(near(total), near(theirs), near(anomaly), near(mine), region_ids)


def solution(mesh):
    cut = ("groups", "cells", "obs")
    in_specs = (P("mem", cut), P(cut), P(cut), P(cut), P(cut, None), P(cut))
    return jax.shard_map(
        body, mesh=mesh, in_specs=in_specs, out_specs=P("mem", cut), check_vma=False
    )
```

```python
import functools

import jax
import jax.numpy as jnp
from jax import lax
from jax.experimental import pallas as pl
from jax.experimental.pallas import tpu as pltpu
from jax.sharding import PartitionSpec as P

NLOC = 4
BLOCK = 512
SUB = 8
LANES = 128
TILE = 256


VMEM = pl.BlockSpec(memory_space=pltpu.VMEM)
SMEM = pl.BlockSpec(memory_space=pltpu.SMEM)
HBM = pl.BlockSpec(memory_space=pl.ANY)


def near(x):
    return pltpu.with_memory_space_constraint(x, pltpu.VMEM)


def prepare_kernel(
    members_hbm, cells_hbm, observed_hbm, error_hbm, noise_hbm, regions_hbm,
    members_ref, onehot_ref, predicted_ref, innov_ref, noise_ref, rows_ref, cells_ref, observed_ref,
    error_ref, all_noise_ref, regions_ref, sems,
):
    moves = [
        pltpu.make_async_copy(src, dst, sems.at[i])
        for i, (src, dst) in enumerate(
            (
                (cells_hbm, cells_ref),
                (members_hbm, members_ref),
                (error_hbm, error_ref),
                (observed_hbm, observed_ref),
                (noise_hbm, all_noise_ref),
                (regions_hbm, regions_ref),
            )
        )
    ]
    for move in moves:
        move.start()
    half, cells = members_ref.shape
    nobs = cells_ref.shape[1]
    moves[0].wait()
    cell = cells_ref[...]
    part = cell // TILE
    onehot = lax.broadcasted_iota(jnp.int32, (TILE, nobs), 0) == cell - part * TILE
    onehot = onehot.astype(jnp.bfloat16)
    onehot_ref[...] = onehot
    moves[1].wait()
    predicted = predict(members_ref, onehot, part)
    predicted_ref[...] = predicted
    moves[2].wait()
    moves[3].wait()
    inverse = 1.0 / error_ref[...]
    moves[4].wait()
    core = lax.axis_index("mem")
    noise = all_noise_ref[pl.ds(pl.multiple_of(core * half, half), half), :].astype(jnp.float32)
    innov = (observed_ref[...] - predicted) * inverse + noise
    innov_ref[...] = innov.astype(jnp.bfloat16)
    noise_ref[...] = all_noise_ref[pl.ds(pl.multiple_of((1 - core) * half, half), half), :]
    moves[5].wait()
    block = cell // BLOCK
    region = jnp.zeros_like(cell)
    for b in range(cells // BLOCK):
        region = jnp.where(block == b, regions_ref[b], region)
    rows_ref[0:1, :] = observed_ref[...]
    rows_ref[1:2, :] = inverse
    rows_ref[2:3, :] = part.astype(jnp.float32)
    rows_ref[3:4, :] = region.astype(jnp.float32)
    rows_ref[4:5, :] = jnp.sum(predicted, axis=0, keepdims=True)
    rows_ref[5:6, :] = jnp.sum(innov * innov, axis=0, keepdims=True)
    rows_ref[6:8, :] = jnp.zeros((2, nobs), jnp.float32)


def predict(members_ref, onehot, part):
    members, cells = members_ref.shape
    tiles = cells // TILE
    stacked = jnp.concatenate(
        [members_ref[:, p * TILE : (p + 1) * TILE] for p in range(tiles)], axis=0
    )
    picked = jnp.dot(stacked, onehot, preferred_element_type=jnp.float32)
    values = picked[0:members]
    for p in range(1, tiles):
        values = jnp.where(part == p, picked[p * members : (p + 1) * members], values)
    return values + 0.2 * values * values * values


def stats_kernel(
    theirs_ref, onehot_ref, predicted_ref, innov_ref, noise_ref, rows_ref,
    sums_ref, sent_ref, half_ref, sens_ref, innovs_ref,
):
    half = theirs_ref.shape[0]
    ne = 2 * half
    pairs = NLOC // 2
    core = lax.axis_index("mem")
    at_mine = pl.ds(pl.multiple_of(core * half, half), half)
    at_theirs = pl.ds(pl.multiple_of((1 - core) * half, half), half)
    observed, inverse, part, region, mine_sum, mine_square = [rows_ref[i : i + 1, :] for i in range(6)]
    mine = predicted_ref[...]
    theirs = predict(theirs_ref, onehot_ref[...], part)
    innov = (observed - theirs) * inverse + noise_ref[...].astype(jnp.float32)
    square = mine_square + jnp.sum(innov * innov, axis=0, keepdims=True)
    pmean = (mine_sum + jnp.sum(theirs, axis=0, keepdims=True)) / ne
    sens_ref[at_mine, :] = ((mine - pmean) * inverse).astype(jnp.bfloat16)
    sens_ref[at_theirs, :] = ((theirs - pmean) * inverse).astype(jnp.bfloat16)
    innovs_ref[at_mine, :] = innov_ref[...]
    innovs_ref[at_theirs, :] = innov.astype(jnp.bfloat16)
    sens = sens_ref[...]
    inside = [region == r for r in range(NLOC)]
    lane = lax.broadcasted_iota(jnp.int32, (SUB, LANES), 1)
    column = lax.broadcasted_iota(jnp.int32, (ne, LANES), 1) % ne
    below = column < lax.broadcasted_iota(jnp.int32, (ne, LANES), 0)
    on_diagonal = column == lax.broadcasted_iota(jnp.int32, (ne, LANES), 0)

    def product(x):
        masked = jnp.concatenate([jnp.where(m, x, jnp.zeros_like(x)) for m in inside], axis=0)
        return lax.dot_general(
            sens, masked, (((1,), (1,)), ((), ())), preferred_element_type=jnp.float32
        )

    gram = product(sens)
    cross = product(innovs_ref[...])
    misfits = [
        jnp.sum(jnp.where(m, square, jnp.float32(0.0)), axis=1, keepdims=True) for m in inside
    ]
    for p in range(pairs):
        lanes = slice(p * LANES, (p + 1) * LANES)
        g = gram[:, lanes]
        row = (1 + p) * ne
        sums_ref[row : row + ne, :] = cross[:, lanes] + g
        tail = (1 + pairs) * ne
        sums_ref[tail + p : tail + p + 1, :] = jnp.where(
            lane < ne, misfits[2 * p], misfits[2 * p + 1]
        )[0:1]
        sums_ref[tail + pairs + p : tail + pairs + p + 1, :] = jnp.sum(
            jnp.where(on_diagonal, g, 0.0), axis=0, keepdims=True
        )
    sums_ref[0:ne, :] = jnp.where(
        on_diagonal, 0.0, jnp.where(below, gram[:, 0:LANES], gram[:, LANES : 2 * LANES])
    )
    pack(sums_ref, sent_ref, half_ref)


def pack(sums_ref, sent_ref, half_ref):
    rows = sums_ref.shape[0] - NLOC
    sent_ref[0:rows, :] = sums_ref[0:rows, :].astype(jnp.bfloat16)
    left = sums_ref[rows : rows + NLOC, :]
    parts = []
    for _ in range(3):
        part = left.astype(jnp.bfloat16).astype(jnp.float32)
        parts.append(part)
        left = left - part
    parts.append(jnp.zeros_like(left))
    tail = jnp.concatenate(parts, axis=0).astype(jnp.bfloat16)
    sent_ref[rows : rows + 4 * NLOC, :] = tail
    half = rows // 2
    start = pl.multiple_of(lax.axis_index("mem") * half, half)
    half_ref[0:half, :] = sums_ref[pl.ds(start, half), :].astype(jnp.bfloat16)
    half_ref[half : half + 4 * NLOC, :] = tail


def fold_kernel(*refs):
    sums_ref, shared_ref, *got, out_ref = refs
    rows = sums_ref.shape[0] - NLOC
    half = rows // 2
    core = lax.axis_index("mem")
    if got:
        out_ref[0:rows, :] = functools.reduce(
            jnp.add, [g[0:rows, :].astype(jnp.float32) for g in got]
        )
    else:
        out_ref[...] = jnp.zeros_like(out_ref)
    mine = pl.ds(pl.multiple_of(core * half, half), half)
    out_ref[mine, :] += sums_ref[mine, :] + shared_ref[0:half, :].astype(jnp.float32)
    tails = [whole(g[rows : rows + 4 * NLOC, :]) for g in got]
    both = sums_ref[rows : rows + NLOC, :] + whole(shared_ref[half : half + 4 * NLOC, :])
    out_ref[rows : rows + NLOC, :] = functools.reduce(
        jnp.add, tails, jnp.where(core == 0, both, jnp.zeros_like(both))
    )


def whole(parts):
    parts = parts.astype(jnp.float32)
    return parts[0:NLOC] + parts[NLOC : 2 * NLOC] + parts[2 * NLOC : 3 * NLOC]


def repack_kernel(mine_ref, theirs_ref, sums_ref, sent_ref, half_ref):
    sums_ref[...] = mine_ref[...] + theirs_ref[...]
    pack(sums_ref, sent_ref, half_ref)


def row_of(x, j):
    return jnp.broadcast_to(x[j : j + 1, :], x.shape)


def lane_of(x, c, lane):
    half = LANES // 2
    index = jnp.where(lane < half, c, half + c)
    return jnp.take_along_axis(x, index, axis=1, mode="promise_in_bounds")


def eliminate(systems, blocks):
    sub = lax.broadcasted_iota(jnp.int32, (SUB, LANES), 0)
    lane = lax.broadcasted_iota(jnp.int32, (SUB, LANES), 1)
    for k in blocks:
        cols = [
            [{i: lane_of(left[i], SUB * k + j, lane) for i in blocks} for j in range(SUB)]
            for left, _ in systems
        ]
        diags = [[col[j][k] for j in range(SUB)] for col in cols]
        panels = [[left[k], right[k]] for left, right in systems]
        scales = [None] * len(systems)
        for j in range(SUB):
            for s, (diag, panel) in enumerate(zip(diags, panels)):
                inverse = 1.0 / row_of(diag[j], j)
                factor = jnp.where(sub == j, 0.0, diag[j]) * inverse
                scales[s] = inverse if j == 0 else jnp.where(sub == j, inverse, scales[s])
                for values, start in ((diag, j + 1), (panel, 0)):
                    for l in range(start, len(values)):
                        values[l] = values[l] - factor * row_of(values[l], j)
        panels = [[x * scale for x in panel] for panel, scale in zip(panels, scales)]
        for (left, right), panel, col in zip(systems, panels, cols):
            for i in blocks:
                if i == k:
                    continue
                for j in range(SUB):
                    left[i] = left[i] - col[j][i] * row_of(panel[0], j)
                    right[i] = right[i] - col[j][i] * row_of(panel[1], j)
            left[k], right[k] = panel


def finish_kernel(
    mine_ref, theirs_ref, anomaly_ref, members_ref, regions_hbm, out_hbm,
    coeff_ref, regions_ref, updated_ref, sems,
):
    half, cells = members_ref.shape
    ne = 2 * half
    count = ne // SUB
    pairs = NLOC // 2
    load = pltpu.make_async_copy(regions_hbm, regions_ref, sems.at[0])
    load.start()

    def total(row, rows=SUB):
        return mine_ref[row : row + rows, :] + theirs_ref[row : row + rows, :]

    lane = lax.broadcasted_iota(jnp.int32, (SUB, LANES), 1)
    sub = lax.broadcasted_iota(jnp.int32, (SUB, LANES), 0)
    tail = total((1 + pairs) * ne, NLOC)
    triangles = total(0, ne)
    turned = triangles.T
    turned = jnp.concatenate([turned[0:ne], turned[ne : 2 * ne]], axis=1)
    systems = []
    for p in range(pairs):
        diagonal = jnp.broadcast_to(tail[pairs + p : pairs + p + 1], (SUB, LANES))
        damped = diagonal + ((ne - 1.0) + jnp.broadcast_to(tail[p : p + 1], (SUB, LANES)) / ne)
        left, right = [], []
        for i in range(count):
            given = (lane % ne < SUB * i + sub) if p == 0 else (lane % ne > SUB * i + sub)
            here = lane % ne == SUB * i + sub
            block = slice(i * SUB, (i + 1) * SUB)
            gram = jnp.where(given, triangles[block], turned[block])
            left.append(jnp.where(here, damped, gram))
            right.append(total((1 + p) * ne + i * SUB) - jnp.where(here, diagonal, gram))
        systems.append((left, right))
    eliminate(systems, range(count))
    for p, (_, right) in enumerate(systems):
        turned = jnp.concatenate(right, axis=0).T
        coeff_ref[2 * p * ne : 2 * (p + 1) * ne, :] = turned.astype(jnp.bfloat16)
    core = lax.axis_index("mem")
    load.wait()
    stores = []
    for b in range(cells // BLOCK):
        start = pl.multiple_of(regions_ref[b] * ne + core * half, half)
        span = slice(b * BLOCK, (b + 1) * BLOCK)
        delta = jnp.dot(
            coeff_ref[pl.ds(start, half), :], anomaly_ref[:, span], preferred_element_type=jnp.float32
        )
        updated_ref[:, span] = (members_ref[:, span].astype(jnp.float32) + delta).astype(jnp.bfloat16)
        stores.append(
            pltpu.make_async_copy(updated_ref.at[:, span], out_hbm.at[:, span], sems.at[1 + b])
        )
        stores[-1].start()
    for store in stores:
        store.wait()


def anomaly_kernel(mine_ref, theirs_ref, out_ref):
    half = mine_ref.shape[0]
    core = lax.axis_index("mem")
    mine = mine_ref[...].astype(jnp.float32)
    theirs = theirs_ref[...].astype(jnp.float32)
    total = jnp.sum(mine, axis=0, keepdims=True) + jnp.sum(theirs, axis=0, keepdims=True)
    center = total / (2 * half)
    at_mine = pl.ds(pl.multiple_of(core * half, half), half)
    at_theirs = pl.ds(pl.multiple_of((1 - core) * half, half), half)
    out_ref[at_mine, :] = (mine - center).astype(jnp.bfloat16)
    out_ref[at_theirs, :] = (theirs - center).astype(jnp.bfloat16)


def stages(sizes):
    bits = [
        [(axis, 1 << i) for i in range(size.bit_length() - 1)] for axis, size in enumerate(sizes)
    ]
    first, last = bits
    groups = []
    while first or last:
        group = first[:2] + last[:1]
        first, last = first[2:], last[1:]
        groups.append(group)
    return groups


PARTNERS = {1: ((), (), 1), 2: ((1,), (3,), 2), 3: ((4, 5, 3), (2, 7, 6), 1)}


def partners(group, sizes):
    low, high, shared = PARTNERS[len(group)]

    def step(mask):
        way = [0, 0]
        for i, (axis, bit) in enumerate(group):
            if mask >> i & 1:
                way[axis] |= bit
        return way

    def place(c, o, m):
        return (c * sizes[1] + o) * 2 + m

    ways = [(step(a), step(b)) for a, b in zip(low, high)] + [(step(shared), step(shared))]
    return [
        [
            (place(c, o, m), place(c ^ way[m][0], o ^ way[m][1], m))
            for c in range(sizes[0])
            for o in range(sizes[1])
            for m in range(2)
        ]
        for way in ways
    ]


def body(members, observed, obs_error, obs_cells, perturbations, region_ids):
    half, cells = members.shape
    ne = 2 * half
    nobs = observed.shape[0]
    blocks = region_ids.shape[0]
    rows = (1 + NLOC // 2) * ne
    swap = [(0, 1), (1, 0)]
    other = lax.ppermute(members, "mem", swap)
    mine, onehot, predicted, innov, noise, lines = pl.pallas_call(
        prepare_kernel,
        out_shape=[
            pltpu.VMEM((half, cells), jnp.bfloat16),
            pltpu.VMEM((TILE, nobs), jnp.bfloat16),
            pltpu.VMEM((half, nobs), jnp.float32),
            pltpu.VMEM((half, nobs), jnp.bfloat16),
            pltpu.VMEM((half, nobs), jnp.bfloat16),
            pltpu.VMEM((SUB, nobs), jnp.float32),
        ],
        in_specs=[HBM] * 6,
        out_specs=[VMEM] * 6,
        scratch_shapes=[
            pltpu.VMEM((1, nobs), jnp.int32),
            pltpu.VMEM((1, nobs), jnp.float32),
            pltpu.VMEM((1, nobs), jnp.float32),
            pltpu.VMEM((ne, nobs), jnp.bfloat16),
            pltpu.SMEM((blocks,), jnp.int32),
            pltpu.SemaphoreType.DMA((6,)),
        ],
        name="prepare",
    )(
        members,
        obs_cells.reshape(1, nobs),
        observed.reshape(1, nobs),
        obs_error.reshape(1, nobs),
        perturbations.T,
        region_ids,
    )
    sums_shape = pltpu.VMEM((rows + NLOC, LANES), jnp.float32)
    packed = [
        sums_shape,
        pltpu.VMEM((rows + 4 * NLOC, LANES), jnp.bfloat16),
        pltpu.VMEM((rows // 2 + 4 * NLOC, LANES), jnp.bfloat16),
    ]
    sums, sent, shared = pl.pallas_call(
        stats_kernel,
        out_shape=packed,
        in_specs=[VMEM] * 6,
        out_specs=[VMEM] * 3,
        scratch_shapes=[pltpu.VMEM((ne, nobs), jnp.bfloat16)] * 2,
        name="stats",
    )(*[near(x) for x in (other, onehot, predicted, innov, noise, lines)])
    anomaly = pl.pallas_call(
        anomaly_kernel,
        out_shape=pltpu.VMEM((ne, cells), jnp.bfloat16),
        in_specs=[VMEM] * 2,
        out_specs=VMEM,
        name="anomaly",
    )(near(mine), near(other))
    axes = ("cells", "obs", "mem")
    sizes = (lax.axis_size("cells"), lax.axis_size("obs"))
    groups = stages(sizes)
    for number, group in enumerate(groups):
        *single, common = partners(group, sizes)
        got = [lax.ppermute(sent, axes, p) for p in single]
        got.insert(0, lax.ppermute(shared, axes, common))
        if number == 0:
            got, anomaly = lax.optimization_barrier((got, anomaly))
        total = pl.pallas_call(
            fold_kernel,
            out_shape=sums_shape,
            in_specs=[VMEM] * (1 + len(got)),
            out_specs=VMEM,
            name="fold",
        )(near(sums), *[near(g) for g in got])
        theirs = lax.ppermute(total, "mem", swap)
        if number < len(groups) - 1:
            sums, sent, shared = pl.pallas_call(
                repack_kernel,
                out_shape=packed,
                in_specs=[VMEM] * 2,
                out_specs=[VMEM] * 3,
                name="repack",
            )(near(total), near(theirs))
    return pl.pallas_call(
        finish_kernel,
        out_shape=jax.ShapeDtypeStruct((half, cells), jnp.bfloat16),
        in_specs=[VMEM] * 4 + [HBM],
        out_specs=HBM,
        scratch_shapes=[
            pltpu.VMEM((NLOC * ne, ne), jnp.bfloat16),
            pltpu.SMEM((blocks,), jnp.int32),
            pltpu.VMEM((half, cells), jnp.bfloat16),
            pltpu.SemaphoreType.DMA((1 + blocks,)),
        ],
        name="finish",
    )(near(total), near(theirs), near(anomaly), near(mine), region_ids)


def solution(mesh):
    cut = ("groups", "cells", "obs")
    in_specs = (P("mem", cut), P(cut), P(cut), P(cut), P(cut, None), P(cut))
    return jax.shard_map(
        body, mesh=mesh, in_specs=in_specs, out_specs=P("mem", cut), check_vma=False
    )
```

```python
import functools

import jax
import jax.numpy as jnp
from jax import lax
from jax.experimental import pallas as pl
from jax.experimental.pallas import tpu as pltpu
from jax.sharding import PartitionSpec as P

NLOC = 4
BLOCK = 512
SUB = 8
LANES = 128
TILE = 256


VMEM = pl.BlockSpec(memory_space=pltpu.VMEM)
SMEM = pl.BlockSpec(memory_space=pltpu.SMEM)
HBM = pl.BlockSpec(memory_space=pl.ANY)


def near(x):
    return pltpu.with_memory_space_constraint(x, pltpu.VMEM)


def prepare_kernel(
    members_hbm, cells_hbm, observed_hbm, error_hbm, noise_hbm, regions_hbm,
    members_ref, onehot_ref, predicted_ref, innov_ref, noise_ref, rows_ref, cells_ref, observed_ref,
    error_ref, all_noise_ref, regions_ref, sems,
):
    moves = [
        pltpu.make_async_copy(src, dst, sems.at[i])
        for i, (src, dst) in enumerate(
            (
                (cells_hbm, cells_ref),
                (members_hbm, members_ref),
                (error_hbm, error_ref),
                (observed_hbm, observed_ref),
                (noise_hbm, all_noise_ref),
                (regions_hbm, regions_ref),
            )
        )
    ]
    for move in moves:
        move.start()
    half, cells = members_ref.shape
    nobs = cells_ref.shape[1]
    place = lax.broadcasted_iota(jnp.int32, (TILE, LANES), 0).astype(jnp.float32).astype(jnp.bfloat16)
    place = jnp.concatenate([place] * (nobs // LANES), axis=1)
    one = jnp.ones((TILE, nobs), jnp.bfloat16)
    moves[0].wait()
    cell = cells_ref[...]
    part = cell // TILE
    within = (cell - part * TILE).astype(jnp.float32).astype(jnp.bfloat16)
    onehot = jnp.where(place == within, one, jnp.zeros_like(one))
    onehot_ref[...] = onehot
    moves[1].wait()
    predicted = predict(members_ref, onehot, part)
    predicted_ref[...] = predicted
    moves[2].wait()
    moves[3].wait()
    inverse = 1.0 / error_ref[...]
    moves[4].wait()
    core = lax.axis_index("mem")
    noise = all_noise_ref[pl.ds(pl.multiple_of(core * half, half), half), :].astype(jnp.float32)
    innov = (observed_ref[...] - predicted) * inverse + noise
    innov_ref[...] = innov.astype(jnp.bfloat16)
    noise_ref[...] = all_noise_ref[pl.ds(pl.multiple_of((1 - core) * half, half), half), :]
    moves[5].wait()
    block = cell // BLOCK
    region = jnp.zeros_like(cell)
    for b in range(cells // BLOCK):
        region = jnp.where(block == b, regions_ref[b], region)
    rows_ref[0:1, :] = observed_ref[...]
    rows_ref[1:2, :] = inverse
    rows_ref[2:3, :] = part.astype(jnp.float32)
    rows_ref[3:4, :] = region.astype(jnp.float32)
    rows_ref[4:5, :] = jnp.sum(predicted, axis=0, keepdims=True)
    rows_ref[5:6, :] = jnp.sum(innov * innov, axis=0, keepdims=True)
    rows_ref[6:8, :] = jnp.zeros((2, nobs), jnp.float32)


def predict(members_ref, onehot, part):
    members, cells = members_ref.shape
    tiles = cells // TILE
    stacked = jnp.concatenate(
        [members_ref[:, p * TILE : (p + 1) * TILE] for p in range(tiles)], axis=0
    )
    picked = jnp.dot(stacked, onehot, preferred_element_type=jnp.float32)
    values = picked[0:members]
    for p in range(1, tiles):
        values = jnp.where(part == p, picked[p * members : (p + 1) * members], values)
    return values + 0.2 * values * values * values


def stats_kernel(
    theirs_ref, onehot_ref, predicted_ref, innov_ref, noise_ref, rows_ref,
    sums_ref, sent_ref, half_ref, sens_ref, innovs_ref,
):
    half = theirs_ref.shape[0]
    ne = 2 * half
    pairs = NLOC // 2
    core = lax.axis_index("mem")
    at_mine = pl.ds(pl.multiple_of(core * half, half), half)
    at_theirs = pl.ds(pl.multiple_of((1 - core) * half, half), half)
    observed, inverse, part, region, mine_sum, mine_square = [rows_ref[i : i + 1, :] for i in range(6)]
    mine = predicted_ref[...]
    theirs = predict(theirs_ref, onehot_ref[...], part)
    innov = (observed - theirs) * inverse + noise_ref[...].astype(jnp.float32)
    square = mine_square + jnp.sum(innov * innov, axis=0, keepdims=True)
    pmean = (mine_sum + jnp.sum(theirs, axis=0, keepdims=True)) / ne
    sens_ref[at_mine, :] = ((mine - pmean) * inverse).astype(jnp.bfloat16)
    sens_ref[at_theirs, :] = ((theirs - pmean) * inverse).astype(jnp.bfloat16)
    innovs_ref[at_mine, :] = innov_ref[...]
    innovs_ref[at_theirs, :] = innov.astype(jnp.bfloat16)
    sens = sens_ref[...]
    inside = [region == r for r in range(NLOC)]
    lane = lax.broadcasted_iota(jnp.int32, (SUB, LANES), 1)
    column = lax.broadcasted_iota(jnp.int32, (ne, LANES), 1) % ne
    below = column < lax.broadcasted_iota(jnp.int32, (ne, LANES), 0)
    on_diagonal = column == lax.broadcasted_iota(jnp.int32, (ne, LANES), 0)

    def product(x):
        masked = jnp.concatenate([jnp.where(m, x, jnp.zeros_like(x)) for m in inside], axis=0)
        return lax.dot_general(
            sens, masked, (((1,), (1,)), ((), ())), preferred_element_type=jnp.float32
        )

    gram = product(sens)
    cross = product(innovs_ref[...])
    misfits = [
        jnp.sum(jnp.where(m, square, jnp.float32(0.0)), axis=1, keepdims=True) for m in inside
    ]
    for p in range(pairs):
        lanes = slice(p * LANES, (p + 1) * LANES)
        g = gram[:, lanes]
        row = (1 + p) * ne
        sums_ref[row : row + ne, :] = cross[:, lanes] + g
        tail = (1 + pairs) * ne
        sums_ref[tail + p : tail + p + 1, :] = jnp.where(
            lane < ne, misfits[2 * p], misfits[2 * p + 1]
        )[0:1]
        sums_ref[tail + pairs + p : tail + pairs + p + 1, :] = jnp.sum(
            jnp.where(on_diagonal, g, 0.0), axis=0, keepdims=True
        )
    sums_ref[0:ne, :] = jnp.where(
        on_diagonal, 0.0, jnp.where(below, gram[:, 0:LANES], gram[:, LANES : 2 * LANES])
    )
    pack(sums_ref, sent_ref, half_ref)


def pack(sums_ref, sent_ref, half_ref):
    rows = sums_ref.shape[0] - NLOC
    sent_ref[0:rows, :] = sums_ref[0:rows, :].astype(jnp.bfloat16)
    left = sums_ref[rows : rows + NLOC, :]
    parts = []
    for _ in range(3):
        part = left.astype(jnp.bfloat16).astype(jnp.float32)
        parts.append(part)
        left = left - part
    parts.append(jnp.zeros_like(left))
    tail = jnp.concatenate(parts, axis=0).astype(jnp.bfloat16)
    sent_ref[rows : rows + 4 * NLOC, :] = tail
    half = rows // 2
    start = pl.multiple_of(lax.axis_index("mem") * half, half)
    half_ref[0:half, :] = sums_ref[pl.ds(start, half), :].astype(jnp.bfloat16)
    half_ref[half : half + 4 * NLOC, :] = tail


def fold_kernel(*refs):
    sums_ref, shared_ref, *got, out_ref = refs
    rows = sums_ref.shape[0] - NLOC
    half = rows // 2
    core = lax.axis_index("mem")
    if got:
        out_ref[0:rows, :] = functools.reduce(
            jnp.add, [g[0:rows, :].astype(jnp.float32) for g in got]
        )
    else:
        out_ref[...] = jnp.zeros_like(out_ref)
    mine = pl.ds(pl.multiple_of(core * half, half), half)
    out_ref[mine, :] += sums_ref[mine, :] + shared_ref[0:half, :].astype(jnp.float32)
    tails = [whole(g[rows : rows + 4 * NLOC, :]) for g in got]
    both = sums_ref[rows : rows + NLOC, :] + whole(shared_ref[half : half + 4 * NLOC, :])
    out_ref[rows : rows + NLOC, :] = functools.reduce(
        jnp.add, tails, jnp.where(core == 0, both, jnp.zeros_like(both))
    )


def whole(parts):
    parts = parts.astype(jnp.float32)
    return parts[0:NLOC] + parts[NLOC : 2 * NLOC] + parts[2 * NLOC : 3 * NLOC]


def repack_kernel(mine_ref, theirs_ref, sums_ref, sent_ref, half_ref):
    sums_ref[...] = mine_ref[...] + theirs_ref[...]
    pack(sums_ref, sent_ref, half_ref)


def row_of(x, j):
    return jnp.broadcast_to(x[j : j + 1, :], x.shape)


def eliminate(systems):
    count = len(systems[0][0])
    sub = lax.broadcasted_iota(jnp.int32, (SUB, LANES), 0)
    lane = lax.broadcasted_iota(jnp.int32, (SUB, LANES), 1)
    first = jnp.where(lane < LANES // 2, 0, LANES // 2)

    def step(k, systems):
        at = [first + (SUB * k + j) for j in range(SUB)]
        spread = [
            [
                [jnp.take_along_axis(x, at[j], axis=1, mode="promise_in_bounds") for x in left]
                for j in range(SUB)
            ]
            for left, _ in systems
        ]
        diags = [[col[j][0] for j in range(SUB)] for col in spread]
        panels = [[left[0], right[0]] for left, right in systems]
        scales = [None] * len(systems)
        for j in range(SUB):
            for s, (diag, panel) in enumerate(zip(diags, panels)):
                inverse = 1.0 / row_of(diag[j], j)
                factor = jnp.where(sub == j, 0.0, diag[j]) * inverse
                scales[s] = inverse if j == 0 else jnp.where(sub == j, inverse, scales[s])
                for values, start in ((diag, j + 1), (panel, 0)):
                    for l in range(start, len(values)):
                        values[l] = values[l] - factor * row_of(values[l], j)
        result = []
        for (left, right), panel, scale, col in zip(systems, panels, scales, spread):
            left, right = list(left), list(right)
            panel = [x * scale for x in panel]
            for i in range(1, count):
                for j in range(SUB):
                    left[i] = left[i] - col[j][i] * row_of(panel[0], j)
                    right[i] = right[i] - col[j][i] * row_of(panel[1], j)
            result.append((left[1:] + panel[:1], right[1:] + panel[1:]))
        return result

    return [right for _, right in lax.fori_loop(0, count, step, systems, unroll=2)]


def finish_kernel(
    mine_ref, theirs_ref, anomaly_ref, members_ref, regions_hbm, out_hbm,
    coeff_ref, regions_ref, updated_ref, sems,
):
    half, cells = members_ref.shape
    ne = 2 * half
    count = ne // SUB
    pairs = NLOC // 2
    load = pltpu.make_async_copy(regions_hbm, regions_ref, sems.at[0])
    load.start()

    def total(row, rows=SUB):
        return mine_ref[row : row + rows, :] + theirs_ref[row : row + rows, :]

    lane = lax.broadcasted_iota(jnp.int32, (SUB, LANES), 1)
    sub = lax.broadcasted_iota(jnp.int32, (SUB, LANES), 0)
    tail = total((1 + pairs) * ne, NLOC)
    triangles = total(0, ne)
    turned = triangles.T
    turned = jnp.concatenate([turned[0:ne], turned[ne : 2 * ne]], axis=1)
    systems = []
    for p in range(pairs):
        diagonal = jnp.broadcast_to(tail[pairs + p : pairs + p + 1], (SUB, LANES))
        damped = diagonal + ((ne - 1.0) + jnp.broadcast_to(tail[p : p + 1], (SUB, LANES)) / ne)
        left, right = [], []
        for i in range(count):
            given = (lane % ne < SUB * i + sub) if p == 0 else (lane % ne > SUB * i + sub)
            here = lane % ne == SUB * i + sub
            block = slice(i * SUB, (i + 1) * SUB)
            gram = jnp.where(given, triangles[block], turned[block])
            left.append(jnp.where(here, damped, gram))
            right.append(total((1 + p) * ne + i * SUB) - jnp.where(here, diagonal, gram))
        systems.append((left, right))
    for p, right in enumerate(eliminate(systems)):
        turned = jnp.concatenate(right, axis=0).T
        coeff_ref[2 * p * ne : 2 * (p + 1) * ne, :] = turned.astype(jnp.bfloat16)
    core = lax.axis_index("mem")
    load.wait()
    stores = []
    for b in range(cells // BLOCK):
        start = pl.multiple_of(regions_ref[b] * ne + core * half, half)
        span = slice(b * BLOCK, (b + 1) * BLOCK)
        delta = jnp.dot(
            coeff_ref[pl.ds(start, half), :], anomaly_ref[:, span], preferred_element_type=jnp.float32
        )
        updated_ref[:, span] = (members_ref[:, span].astype(jnp.float32) + delta).astype(jnp.bfloat16)
        stores.append(
            pltpu.make_async_copy(updated_ref.at[:, span], out_hbm.at[:, span], sems.at[1 + b])
        )
        stores[-1].start()
    for store in stores:
        store.wait()


def anomaly_kernel(mine_ref, theirs_ref, out_ref):
    half = mine_ref.shape[0]
    core = lax.axis_index("mem")
    mine = mine_ref[...].astype(jnp.float32)
    theirs = theirs_ref[...].astype(jnp.float32)
    total = jnp.sum(mine, axis=0, keepdims=True) + jnp.sum(theirs, axis=0, keepdims=True)
    center = total / (2 * half)
    at_mine = pl.ds(pl.multiple_of(core * half, half), half)
    at_theirs = pl.ds(pl.multiple_of((1 - core) * half, half), half)
    out_ref[at_mine, :] = (mine - center).astype(jnp.bfloat16)
    out_ref[at_theirs, :] = (theirs - center).astype(jnp.bfloat16)


def stages(sizes):
    bits = [
        [(axis, 1 << i) for i in range(size.bit_length() - 1)] for axis, size in enumerate(sizes)
    ]
    first, last = bits
    groups = []
    while first or last:
        group = first[:2] + last[:1]
        first, last = first[2:], last[1:]
        groups.append(group)
    return groups


PARTNERS = {1: ((), (), 1), 2: ((1,), (3,), 2), 3: ((4, 3, 2), (5, 7, 6), 1)}


def partners(group, sizes):
    low, high, shared = PARTNERS[len(group)]

    def step(mask):
        way = [0, 0]
        for i, (axis, bit) in enumerate(group):
            if mask >> i & 1:
                way[axis] |= bit
        return way

    def place(c, o, m):
        return (c * sizes[1] + o) * 2 + m

    ways = [(step(a), step(b)) for a, b in zip(low, high)] + [(step(shared), step(shared))]
    return [
        [
            (place(c, o, m), place(c ^ way[m][0], o ^ way[m][1], m))
            for c in range(sizes[0])
            for o in range(sizes[1])
            for m in range(2)
        ]
        for way in ways
    ]


def body(members, observed, obs_error, obs_cells, perturbations, region_ids):
    half, cells = members.shape
    ne = 2 * half
    nobs = observed.shape[0]
    blocks = region_ids.shape[0]
    rows = (1 + NLOC // 2) * ne
    swap = [(0, 1), (1, 0)]
    other = lax.ppermute(members, "mem", swap)
    mine, onehot, predicted, innov, noise, lines = pl.pallas_call(
        prepare_kernel,
        out_shape=[
            pltpu.VMEM((half, cells), jnp.bfloat16),
            pltpu.VMEM((TILE, nobs), jnp.bfloat16),
            pltpu.VMEM((half, nobs), jnp.float32),
            pltpu.VMEM((half, nobs), jnp.bfloat16),
            pltpu.VMEM((half, nobs), jnp.bfloat16),
            pltpu.VMEM((SUB, nobs), jnp.float32),
        ],
        in_specs=[HBM] * 6,
        out_specs=[VMEM] * 6,
        scratch_shapes=[
            pltpu.VMEM((1, nobs), jnp.int32),
            pltpu.VMEM((1, nobs), jnp.float32),
            pltpu.VMEM((1, nobs), jnp.float32),
            pltpu.VMEM((ne, nobs), jnp.bfloat16),
            pltpu.SMEM((blocks,), jnp.int32),
            pltpu.SemaphoreType.DMA((6,)),
        ],
        name="prepare",
    )(
        members,
        obs_cells.reshape(1, nobs),
        observed.reshape(1, nobs),
        obs_error.reshape(1, nobs),
        perturbations.T,
        region_ids,
    )
    sums_shape = pltpu.VMEM((rows + NLOC, LANES), jnp.float32)
    packed = [
        sums_shape,
        pltpu.VMEM((rows + 4 * NLOC, LANES), jnp.bfloat16),
        pltpu.VMEM((rows // 2 + 4 * NLOC, LANES), jnp.bfloat16),
    ]
    sums, sent, shared = pl.pallas_call(
        stats_kernel,
        out_shape=packed,
        in_specs=[VMEM] * 6,
        out_specs=[VMEM] * 3,
        scratch_shapes=[pltpu.VMEM((ne, nobs), jnp.bfloat16)] * 2,
        name="stats",
    )(*[near(x) for x in (other, onehot, predicted, innov, noise, lines)])
    anomaly = pl.pallas_call(
        anomaly_kernel,
        out_shape=pltpu.VMEM((ne, cells), jnp.bfloat16),
        in_specs=[VMEM] * 2,
        out_specs=VMEM,
        name="anomaly",
    )(near(mine), near(other))
    axes = ("cells", "obs", "mem")
    sizes = (lax.axis_size("cells"), lax.axis_size("obs"))
    groups = stages(sizes)
    for number, group in enumerate(groups):
        *single, common = partners(group, sizes)
        got = [lax.ppermute(sent, axes, p) for p in single]
        got.insert(0, lax.ppermute(shared, axes, common))
        if number == 0:
            got, anomaly = lax.optimization_barrier((got, anomaly))
        total = pl.pallas_call(
            fold_kernel,
            out_shape=sums_shape,
            in_specs=[VMEM] * (1 + len(got)),
            out_specs=VMEM,
            name="fold",
        )(near(sums), *[near(g) for g in got])
        theirs = lax.ppermute(total, "mem", swap)
        if number < len(groups) - 1:
            sums, sent, shared = pl.pallas_call(
                repack_kernel,
                out_shape=packed,
                in_specs=[VMEM] * 2,
                out_specs=[VMEM] * 3,
                name="repack",
            )(near(total), near(theirs))
    return pl.pallas_call(
        finish_kernel,
        out_shape=jax.ShapeDtypeStruct((half, cells), jnp.bfloat16),
        in_specs=[VMEM] * 4 + [HBM],
        out_specs=HBM,
        scratch_shapes=[
            pltpu.VMEM((NLOC * ne, ne), jnp.bfloat16),
            pltpu.SMEM((blocks,), jnp.int32),
            pltpu.VMEM((half, cells), jnp.bfloat16),
            pltpu.SemaphoreType.DMA((1 + blocks,)),
        ],
        name="finish",
    )(near(total), near(theirs), near(anomaly), near(mine), region_ids)


def solution(mesh):
    cut = ("groups", "cells", "obs")
    in_specs = (P("mem", cut), P(cut), P(cut), P(cut), P(cut, None), P(cut))
    return jax.shard_map(
        body, mesh=mesh, in_specs=in_specs, out_specs=P("mem", cut), check_vma=False
    )
```

```python
import functools

import jax
import jax.numpy as jnp
from jax import lax
from jax.experimental import pallas as pl
from jax.experimental.pallas import tpu as pltpu
from jax.sharding import PartitionSpec as P

NLOC = 4
BLOCK = 512
SUB = 8
LANES = 128
TILE = 256


VMEM = pl.BlockSpec(memory_space=pltpu.VMEM)
SMEM = pl.BlockSpec(memory_space=pltpu.SMEM)
HBM = pl.BlockSpec(memory_space=pl.ANY)


def near(x):
    return pltpu.with_memory_space_constraint(x, pltpu.VMEM)


def prepare_kernel(
    members_hbm, cells_hbm, observed_hbm, error_hbm, noise_hbm, regions_hbm,
    members_ref, onehot_ref, predicted_ref, innov_ref, noise_ref, rows_ref, cells_ref, observed_ref,
    error_ref, all_noise_ref, regions_ref, sems,
):
    moves = [
        pltpu.make_async_copy(src, dst, sems.at[i])
        for i, (src, dst) in enumerate(
            (
                (cells_hbm, cells_ref),
                (members_hbm, members_ref),
                (error_hbm, error_ref),
                (observed_hbm, observed_ref),
                (noise_hbm, all_noise_ref),
                (regions_hbm, regions_ref),
            )
        )
    ]
    for move in moves:
        move.start()
    half, cells = members_ref.shape
    nobs = cells_ref.shape[1]
    place = lax.broadcasted_iota(jnp.int32, (TILE, LANES), 0).astype(jnp.float32).astype(jnp.bfloat16)
    place = jnp.concatenate([place] * (nobs // LANES), axis=1)
    one = jnp.ones((TILE, nobs), jnp.bfloat16)
    moves[0].wait()
    cell = cells_ref[...]
    part = cell // TILE
    within = (cell - part * TILE).astype(jnp.float32).astype(jnp.bfloat16)
    onehot = jnp.where(place == within, one, jnp.zeros_like(one))
    onehot_ref[...] = onehot
    moves[1].wait()
    predicted = predict(members_ref, onehot, part)
    predicted_ref[...] = predicted
    moves[2].wait()
    moves[3].wait()
    inverse = 1.0 / error_ref[...]
    moves[4].wait()
    core = lax.axis_index("mem")
    noise = all_noise_ref[pl.ds(pl.multiple_of(core * half, half), half), :].astype(jnp.float32)
    innov = (observed_ref[...] - predicted) * inverse + noise
    innov_ref[...] = innov.astype(jnp.bfloat16)
    noise_ref[...] = all_noise_ref[pl.ds(pl.multiple_of((1 - core) * half, half), half), :]
    moves[5].wait()
    block = cell // BLOCK
    region = jnp.zeros_like(cell)
    for b in range(cells // BLOCK):
        region = jnp.where(block == b, regions_ref[b], region)
    rows_ref[0:1, :] = observed_ref[...]
    rows_ref[1:2, :] = inverse
    rows_ref[2:3, :] = part.astype(jnp.float32)
    rows_ref[3:4, :] = region.astype(jnp.float32)
    rows_ref[4:5, :] = jnp.sum(predicted, axis=0, keepdims=True)
    rows_ref[5:6, :] = jnp.sum(innov * innov, axis=0, keepdims=True)
    rows_ref[6:8, :] = jnp.zeros((2, nobs), jnp.float32)


def predict(members_ref, onehot, part):
    members, cells = members_ref.shape
    tiles = cells // TILE
    stacked = jnp.concatenate(
        [members_ref[:, p * TILE : (p + 1) * TILE] for p in range(tiles)], axis=0
    )
    picked = jnp.dot(stacked, onehot, preferred_element_type=jnp.float32)
    values = picked[0:members]
    for p in range(1, tiles):
        values = jnp.where(part == p, picked[p * members : (p + 1) * members], values)
    return values + 0.2 * values * values * values


def stats_kernel(
    theirs_ref, onehot_ref, predicted_ref, innov_ref, noise_ref, rows_ref,
    sums_ref, half_ref, sens_ref, innovs_ref,
):
    half = theirs_ref.shape[0]
    ne = 2 * half
    pairs = NLOC // 2
    core = lax.axis_index("mem")
    at_mine = pl.ds(pl.multiple_of(core * half, half), half)
    at_theirs = pl.ds(pl.multiple_of((1 - core) * half, half), half)
    observed, inverse, part, region, mine_sum, mine_square = [rows_ref[i : i + 1, :] for i in range(6)]
    mine = predicted_ref[...]
    theirs = predict(theirs_ref, onehot_ref[...], part)
    innov = (observed - theirs) * inverse + noise_ref[...].astype(jnp.float32)
    square = mine_square + jnp.sum(innov * innov, axis=0, keepdims=True)
    pmean = (mine_sum + jnp.sum(theirs, axis=0, keepdims=True)) / ne
    sens_ref[at_mine, :] = ((mine - pmean) * inverse).astype(jnp.bfloat16)
    sens_ref[at_theirs, :] = ((theirs - pmean) * inverse).astype(jnp.bfloat16)
    innovs_ref[at_mine, :] = innov_ref[...]
    innovs_ref[at_theirs, :] = innov.astype(jnp.bfloat16)
    sens = sens_ref[...]
    inside = [region == r for r in range(NLOC)]
    lane = lax.broadcasted_iota(jnp.int32, (SUB, LANES), 1)
    column = lax.broadcasted_iota(jnp.int32, (ne, LANES), 1) % ne
    below = column < lax.broadcasted_iota(jnp.int32, (ne, LANES), 0)
    on_diagonal = column == lax.broadcasted_iota(jnp.int32, (ne, LANES), 0)

    def product(x):
        masked = jnp.concatenate([jnp.where(m, x, jnp.zeros_like(x)) for m in inside], axis=0)
        return lax.dot_general(
            sens, masked, (((1,), (1,)), ((), ())), preferred_element_type=jnp.float32
        )

    gram = product(sens)
    cross = product(innovs_ref[...])
    misfits = [
        jnp.sum(jnp.where(m, square, jnp.float32(0.0)), axis=1, keepdims=True) for m in inside
    ]
    for p in range(pairs):
        lanes = slice(p * LANES, (p + 1) * LANES)
        g = gram[:, lanes]
        row = (1 + p) * ne
        sums_ref[row : row + ne, :] = cross[:, lanes] + g
        tail = (1 + pairs) * ne
        sums_ref[tail + p : tail + p + 1, :] = jnp.where(
            lane < ne, misfits[2 * p], misfits[2 * p + 1]
        )[0:1]
        sums_ref[tail + pairs + p : tail + pairs + p + 1, :] = jnp.sum(
            jnp.where(on_diagonal, g, 0.0), axis=0, keepdims=True
        )
    sums_ref[0:ne, :] = jnp.where(
        on_diagonal, 0.0, jnp.where(below, gram[:, 0:LANES], gram[:, LANES : 2 * LANES])
    )
    sums_ref[tail + 2 * pairs : tail + SUB, :] = jnp.zeros((SUB - 2 * pairs, LANES), jnp.float32)
    pick_half(sums_ref, half_ref)


def pick_half(sums_ref, half_ref):
    rows = sums_ref.shape[0] - SUB
    half = rows // 2
    start = pl.multiple_of(lax.axis_index("mem") * half, half)
    half_ref[0:half, :] = sums_ref[pl.ds(start, half), :]
    half_ref[half : half + SUB, :] = sums_ref[rows : rows + SUB, :]


def fold_kernel(*refs):
    sums_ref, shared_ref, *got, out_ref = refs
    rows = sums_ref.shape[0] - SUB
    half = rows // 2
    core = lax.axis_index("mem")
    if got:
        out_ref[...] = functools.reduce(jnp.add, [g[...] for g in got])
    else:
        out_ref[...] = jnp.zeros_like(out_ref)
    mine = pl.ds(pl.multiple_of(core * half, half), half)
    out_ref[mine, :] += sums_ref[mine, :] + shared_ref[0:half, :]
    both = sums_ref[rows : rows + SUB, :] + shared_ref[half : half + SUB, :]
    out_ref[rows : rows + SUB, :] += jnp.where(core == 0, both, jnp.zeros_like(both))


def repack_kernel(mine_ref, theirs_ref, sums_ref, half_ref):
    sums_ref[...] = mine_ref[...] + theirs_ref[...]
    pick_half(sums_ref, half_ref)


def row_of(x, j):
    return jnp.broadcast_to(x[j : j + 1, :], x.shape)


def eliminate(systems):
    count = len(systems[0][0])
    sub = lax.broadcasted_iota(jnp.int32, (SUB, LANES), 0)
    lane = lax.broadcasted_iota(jnp.int32, (SUB, LANES), 1)
    first = jnp.where(lane < LANES // 2, 0, LANES // 2)

    def step(k, systems):
        at = [first + (SUB * k + j) for j in range(SUB)]
        spread = [
            [
                [jnp.take_along_axis(x, at[j], axis=1, mode="promise_in_bounds") for x in left]
                for j in range(SUB)
            ]
            for left, _ in systems
        ]
        diags = [[col[j][0] for j in range(SUB)] for col in spread]
        panels = [[left[0], right[0]] for left, right in systems]
        scales = [None] * len(systems)
        for j in range(SUB):
            for s, (diag, panel) in enumerate(zip(diags, panels)):
                inverse = 1.0 / row_of(diag[j], j)
                factor = jnp.where(sub == j, 0.0, diag[j]) * inverse
                scales[s] = inverse if j == 0 else jnp.where(sub == j, inverse, scales[s])
                for values, start in ((diag, j + 1), (panel, 0)):
                    for l in range(start, len(values)):
                        values[l] = values[l] - factor * row_of(values[l], j)
        result = []
        for (left, right), panel, scale, col in zip(systems, panels, scales, spread):
            left, right = list(left), list(right)
            panel = [x * scale for x in panel]
            for i in range(1, count):
                for j in range(SUB):
                    left[i] = left[i] - col[j][i] * row_of(panel[0], j)
                    right[i] = right[i] - col[j][i] * row_of(panel[1], j)
            result.append((left[1:] + panel[:1], right[1:] + panel[1:]))
        return result

    return [right for _, right in lax.fori_loop(0, count, step, systems, unroll=2)]


def finish_kernel(
    mine_ref, theirs_ref, anomaly_ref, members_ref, regions_hbm, out_hbm,
    coeff_ref, regions_ref, updated_ref, sems,
):
    half, cells = members_ref.shape
    ne = 2 * half
    count = ne // SUB
    pairs = NLOC // 2
    load = pltpu.make_async_copy(regions_hbm, regions_ref, sems.at[0])
    load.start()

    def total(row, rows=SUB):
        return mine_ref[row : row + rows, :] + theirs_ref[row : row + rows, :]

    lane = lax.broadcasted_iota(jnp.int32, (SUB, LANES), 1)
    sub = lax.broadcasted_iota(jnp.int32, (SUB, LANES), 0)
    tail = total((1 + pairs) * ne)
    triangles = total(0, ne)
    turned = triangles.T
    turned = jnp.concatenate([turned[0:ne], turned[ne : 2 * ne]], axis=1)
    systems = []
    for p in range(pairs):
        diagonal = jnp.broadcast_to(tail[pairs + p : pairs + p + 1], (SUB, LANES))
        damped = diagonal + ((ne - 1.0) + jnp.broadcast_to(tail[p : p + 1], (SUB, LANES)) / ne)
        left, right = [], []
        for i in range(count):
            given = (lane % ne < SUB * i + sub) if p == 0 else (lane % ne > SUB * i + sub)
            here = lane % ne == SUB * i + sub
            block = slice(i * SUB, (i + 1) * SUB)
            gram = jnp.where(given, triangles[block], turned[block])
            left.append(jnp.where(here, damped, gram))
            right.append(total((1 + p) * ne + i * SUB) - jnp.where(here, diagonal, gram))
        systems.append((left, right))
    for p, right in enumerate(eliminate(systems)):
        turned = jnp.concatenate(right, axis=0).T
        coeff_ref[2 * p * ne : 2 * (p + 1) * ne, :] = turned.astype(jnp.bfloat16)
    core = lax.axis_index("mem")
    load.wait()
    stores = []
    for b in range(cells // BLOCK):
        start = pl.multiple_of(regions_ref[b] * ne + core * half, half)
        span = slice(b * BLOCK, (b + 1) * BLOCK)
        delta = jnp.dot(
            coeff_ref[pl.ds(start, half), :], anomaly_ref[:, span], preferred_element_type=jnp.float32
        )
        updated_ref[:, span] = (members_ref[:, span].astype(jnp.float32) + delta).astype(jnp.bfloat16)
        stores.append(
            pltpu.make_async_copy(updated_ref.at[:, span], out_hbm.at[:, span], sems.at[1 + b])
        )
        stores[-1].start()
    for store in stores:
        store.wait()


def anomaly_kernel(mine_ref, theirs_ref, out_ref):
    half = mine_ref.shape[0]
    core = lax.axis_index("mem")
    mine = mine_ref[...].astype(jnp.float32)
    theirs = theirs_ref[...].astype(jnp.float32)
    total = jnp.sum(mine, axis=0, keepdims=True) + jnp.sum(theirs, axis=0, keepdims=True)
    center = total / (2 * half)
    at_mine = pl.ds(pl.multiple_of(core * half, half), half)
    at_theirs = pl.ds(pl.multiple_of((1 - core) * half, half), half)
    out_ref[at_mine, :] = (mine - center).astype(jnp.bfloat16)
    out_ref[at_theirs, :] = (theirs - center).astype(jnp.bfloat16)


def stages(sizes):
    bits = [
        [(axis, 1 << i) for i in range(size.bit_length() - 1)] for axis, size in enumerate(sizes)
    ]
    first, last = bits
    groups = []
    while first or last:
        group = first[:2] + last[:1]
        first, last = first[2:], last[1:]
        groups.append(group)
    return groups


PARTNERS = {1: ((), (), 1), 2: ((1,), (3,), 2), 3: ((4, 3, 2), (5, 7, 6), 1)}


def partners(group, sizes):
    low, high, shared = PARTNERS[len(group)]

    def step(mask):
        way = [0, 0]
        for i, (axis, bit) in enumerate(group):
            if mask >> i & 1:
                way[axis] |= bit
        return way

    def place(c, o, m):
        return (c * sizes[1] + o) * 2 + m

    ways = [(step(a), step(b)) for a, b in zip(low, high)] + [(step(shared), step(shared))]
    return [
        [
            (place(c, o, m), place(c ^ way[m][0], o ^ way[m][1], m))
            for c in range(sizes[0])
            for o in range(sizes[1])
            for m in range(2)
        ]
        for way in ways
    ]


def body(members, observed, obs_error, obs_cells, perturbations, region_ids):
    half, cells = members.shape
    ne = 2 * half
    nobs = observed.shape[0]
    blocks = region_ids.shape[0]
    rows = (1 + NLOC // 2) * ne
    swap = [(0, 1), (1, 0)]
    other = lax.ppermute(members, "mem", swap)
    mine, onehot, predicted, innov, noise, lines = pl.pallas_call(
        prepare_kernel,
        out_shape=[
            pltpu.VMEM((half, cells), jnp.bfloat16),
            pltpu.VMEM((TILE, nobs), jnp.bfloat16),
            pltpu.VMEM((half, nobs), jnp.float32),
            pltpu.VMEM((half, nobs), jnp.bfloat16),
            pltpu.VMEM((half, nobs), jnp.bfloat16),
            pltpu.VMEM((SUB, nobs), jnp.float32),
        ],
        in_specs=[HBM] * 6,
        out_specs=[VMEM] * 6,
        scratch_shapes=[
            pltpu.VMEM((1, nobs), jnp.int32),
            pltpu.VMEM((1, nobs), jnp.float32),
            pltpu.VMEM((1, nobs), jnp.float32),
            pltpu.VMEM((ne, nobs), jnp.bfloat16),
            pltpu.SMEM((blocks,), jnp.int32),
            pltpu.SemaphoreType.DMA((6,)),
        ],
        name="prepare",
    )(
        members,
        obs_cells.reshape(1, nobs),
        observed.reshape(1, nobs),
        obs_error.reshape(1, nobs),
        perturbations.T,
        region_ids,
    )
    sums_shape = pltpu.VMEM((rows + SUB, LANES), jnp.float32)
    packed = [sums_shape, pltpu.VMEM((rows // 2 + SUB, LANES), jnp.float32)]
    sums, shared = pl.pallas_call(
        stats_kernel,
        out_shape=packed,
        in_specs=[VMEM] * 6,
        out_specs=[VMEM] * 2,
        scratch_shapes=[pltpu.VMEM((ne, nobs), jnp.bfloat16)] * 2,
        name="stats",
    )(*[near(x) for x in (other, onehot, predicted, innov, noise, lines)])
    anomaly = pl.pallas_call(
        anomaly_kernel,
        out_shape=pltpu.VMEM((ne, cells), jnp.bfloat16),
        in_specs=[VMEM] * 2,
        out_specs=VMEM,
        name="anomaly",
    )(near(mine), near(other))
    axes = ("cells", "obs", "mem")
    sizes = (lax.axis_size("cells"), lax.axis_size("obs"))
    groups = stages(sizes)
    for number, group in enumerate(groups):
        *single, common = partners(group, sizes)
        got = [lax.ppermute(sums, axes, p) for p in single]
        got.insert(0, lax.ppermute(shared, axes, common))
        if number == 0:
            got, anomaly = lax.optimization_barrier((got, anomaly))
        total = pl.pallas_call(
            fold_kernel,
            out_shape=sums_shape,
            in_specs=[VMEM] * (1 + len(got)),
            out_specs=VMEM,
            name="fold",
        )(near(sums), *[near(g) for g in got])
        theirs = lax.ppermute(total, "mem", swap)
        if number < len(groups) - 1:
            sums, shared = pl.pallas_call(
                repack_kernel,
                out_shape=packed,
                in_specs=[VMEM] * 2,
                out_specs=[VMEM] * 2,
                name="repack",
            )(near(total), near(theirs))
    return pl.pallas_call(
        finish_kernel,
        out_shape=jax.ShapeDtypeStruct((half, cells), jnp.bfloat16),
        in_specs=[VMEM] * 4 + [HBM],
        out_specs=HBM,
        scratch_shapes=[
            pltpu.VMEM((NLOC * ne, ne), jnp.bfloat16),
            pltpu.SMEM((blocks,), jnp.int32),
            pltpu.VMEM((half, cells), jnp.bfloat16),
            pltpu.SemaphoreType.DMA((1 + blocks,)),
        ],
        name="finish",
    )(near(total), near(theirs), near(anomaly), near(mine), region_ids)


def solution(mesh):
    cut = ("groups", "cells", "obs")
    in_specs = (P("mem", cut), P(cut), P(cut), P(cut), P(cut, None), P(cut))
    return jax.shard_map(
        body, mesh=mesh, in_specs=in_specs, out_specs=P("mem", cut), check_vma=False
    )
```

```python
import functools

import jax
import jax.numpy as jnp
from jax import lax
from jax.experimental import pallas as pl
from jax.experimental.pallas import tpu as pltpu
from jax.sharding import PartitionSpec as P

NLOC = 4
BLOCK = 512
SUB = 8
LANES = 128
TILE = 256


VMEM = pl.BlockSpec(memory_space=pltpu.VMEM)
SMEM = pl.BlockSpec(memory_space=pltpu.SMEM)
HBM = pl.BlockSpec(memory_space=pl.ANY)


def near(x):
    return pltpu.with_memory_space_constraint(x, pltpu.VMEM)


def prepare_kernel(
    members_hbm, cells_hbm, observed_hbm, error_hbm, noise_hbm, regions_hbm,
    members_ref, onehot_ref, predicted_ref, innov_ref, noise_ref, rows_ref, cells_ref, observed_ref,
    error_ref, all_noise_ref, regions_ref, sems,
):
    moves = [
        pltpu.make_async_copy(src, dst, sems.at[i])
        for i, (src, dst) in enumerate(
            (
                (cells_hbm, cells_ref),
                (members_hbm, members_ref),
                (error_hbm, error_ref),
                (observed_hbm, observed_ref),
                (noise_hbm, all_noise_ref),
                (regions_hbm, regions_ref),
            )
        )
    ]
    for move in moves:
        move.start()
    half, cells = members_ref.shape
    nobs = cells_ref.shape[1]
    place = lax.broadcasted_iota(jnp.int32, (TILE, LANES), 0).astype(jnp.float32).astype(jnp.bfloat16)
    place = jnp.concatenate([place] * (nobs // LANES), axis=1)
    one = jnp.ones((TILE, nobs), jnp.bfloat16)
    moves[0].wait()
    cell = cells_ref[...]
    part = cell // TILE
    within = (cell - part * TILE).astype(jnp.float32).astype(jnp.bfloat16)
    onehot = jnp.where(place == within, one, jnp.zeros_like(one))
    onehot_ref[...] = onehot
    moves[1].wait()
    predicted = predict(members_ref, onehot, part)
    predicted_ref[...] = predicted
    moves[2].wait()
    moves[3].wait()
    inverse = 1.0 / error_ref[...]
    moves[4].wait()
    core = lax.axis_index("mem")
    noise = all_noise_ref[pl.ds(pl.multiple_of(core * half, half), half), :].astype(jnp.float32)
    innov = (observed_ref[...] - predicted) * inverse + noise
    innov_ref[...] = innov.astype(jnp.bfloat16)
    noise_ref[...] = all_noise_ref[pl.ds(pl.multiple_of((1 - core) * half, half), half), :]
    moves[5].wait()
    block = cell // BLOCK
    region = jnp.zeros_like(cell)
    for b in range(cells // BLOCK):
        region = jnp.where(block == b, regions_ref[b], region)
    rows_ref[0:1, :] = observed_ref[...]
    rows_ref[1:2, :] = inverse
    rows_ref[2:3, :] = part.astype(jnp.float32)
    rows_ref[3:4, :] = region.astype(jnp.float32)
    rows_ref[4:5, :] = jnp.sum(predicted, axis=0, keepdims=True)
    rows_ref[5:6, :] = jnp.sum(innov * innov, axis=0, keepdims=True)
    rows_ref[6:8, :] = jnp.zeros((2, nobs), jnp.float32)


def predict(members_ref, onehot, part):
    members, cells = members_ref.shape
    tiles = cells // TILE
    stacked = jnp.concatenate(
        [members_ref[:, p * TILE : (p + 1) * TILE] for p in range(tiles)], axis=0
    )
    picked = jnp.dot(stacked, onehot, preferred_element_type=jnp.float32)
    values = picked[0:members]
    for p in range(1, tiles):
        values = jnp.where(part == p, picked[p * members : (p + 1) * members], values)
    return values + 0.2 * values * values * values


def stats_kernel(
    theirs_ref, onehot_ref, predicted_ref, innov_ref, noise_ref, rows_ref,
    sums_ref, sent_ref, half_ref, sens_ref, innovs_ref,
):
    half = theirs_ref.shape[0]
    ne = 2 * half
    pairs = NLOC // 2
    core = lax.axis_index("mem")
    at_mine = pl.ds(pl.multiple_of(core * half, half), half)
    at_theirs = pl.ds(pl.multiple_of((1 - core) * half, half), half)
    observed, inverse, part, region, mine_sum, mine_square = [rows_ref[i : i + 1, :] for i in range(6)]
    mine = predicted_ref[...]
    theirs = predict(theirs_ref, onehot_ref[...], part)
    innov = (observed - theirs) * inverse + noise_ref[...].astype(jnp.float32)
    square = mine_square + jnp.sum(innov * innov, axis=0, keepdims=True)
    pmean = (mine_sum + jnp.sum(theirs, axis=0, keepdims=True)) / ne
    sens_ref[at_mine, :] = ((mine - pmean) * inverse).astype(jnp.bfloat16)
    sens_ref[at_theirs, :] = ((theirs - pmean) * inverse).astype(jnp.bfloat16)
    innovs_ref[at_mine, :] = innov_ref[...]
    innovs_ref[at_theirs, :] = innov.astype(jnp.bfloat16)
    sens = sens_ref[...]
    inside = [region == r for r in range(NLOC)]
    lane = lax.broadcasted_iota(jnp.int32, (SUB, LANES), 1)
    column = lax.broadcasted_iota(jnp.int32, (ne, LANES), 1) % ne
    below = column < lax.broadcasted_iota(jnp.int32, (ne, LANES), 0)
    on_diagonal = column == lax.broadcasted_iota(jnp.int32, (ne, LANES), 0)

    def product(x):
        masked = jnp.concatenate([jnp.where(m, x, jnp.zeros_like(x)) for m in inside], axis=0)
        return lax.dot_general(
            sens, masked, (((1,), (1,)), ((), ())), preferred_element_type=jnp.float32
        )

    gram = product(sens)
    cross = product(innovs_ref[...])
    misfits = [
        jnp.sum(jnp.where(m, square, jnp.float32(0.0)), axis=1, keepdims=True) for m in inside
    ]
    for p in range(pairs):
        lanes = slice(p * LANES, (p + 1) * LANES)
        g = gram[:, lanes]
        row = (1 + p) * ne
        sums_ref[row : row + ne, :] = cross[:, lanes] + g
        tail = (1 + pairs) * ne
        sums_ref[tail + p : tail + p + 1, :] = jnp.where(
            lane < ne, misfits[2 * p], misfits[2 * p + 1]
        )[0:1]
        sums_ref[tail + pairs + p : tail + pairs + p + 1, :] = jnp.sum(
            jnp.where(on_diagonal, g, 0.0), axis=0, keepdims=True
        )
    sums_ref[0:ne, :] = jnp.where(
        on_diagonal, 0.0, jnp.where(below, gram[:, 0:LANES], gram[:, LANES : 2 * LANES])
    )
    sums_ref[tail + 2 * pairs : tail + SUB, :] = jnp.zeros((SUB - 2 * pairs, LANES), jnp.float32)
    pack(sums_ref, sent_ref, half_ref)


def pack(sums_ref, sent_ref, half_ref):
    rows = sums_ref.shape[0] - SUB
    ne = rows // (1 + NLOC // 2)
    sent_ref[0:rows, :] = sums_ref[0:rows, :].astype(jnp.bfloat16)
    triangles = sums_ref[0:ne, :]
    rest = triangles - triangles.astype(jnp.bfloat16).astype(jnp.float32)
    sent_ref[rows : rows + ne, :] = rest.astype(jnp.bfloat16)
    left = sums_ref[rows : rows + NLOC, :]
    parts = []
    for _ in range(3):
        part = left.astype(jnp.bfloat16).astype(jnp.float32)
        parts.append(part)
        left = left - part
    parts.append(jnp.zeros_like(left))
    sent_ref[rows + ne : rows + ne + 4 * NLOC, :] = jnp.concatenate(parts, axis=0).astype(jnp.bfloat16)
    pick_half(sums_ref, half_ref)


def pick_half(sums_ref, half_ref):
    rows = sums_ref.shape[0] - SUB
    half = rows // 2
    start = pl.multiple_of(lax.axis_index("mem") * half, half)
    half_ref[0:half, :] = sums_ref[pl.ds(start, half), :]
    half_ref[half : half + SUB, :] = sums_ref[rows : rows + SUB, :]


def fold_kernel(*refs):
    sums_ref, shared_ref, *got, out_ref = refs
    rows = sums_ref.shape[0] - SUB
    half = rows // 2
    core = lax.axis_index("mem")
    ne = rows // (1 + NLOC // 2)
    out_ref[...] = jnp.zeros_like(out_ref)
    if got:
        wide = [g[...].astype(jnp.float32) for g in got]
        out_ref[0:rows, :] = functools.reduce(jnp.add, [g[0:rows] for g in wide])
        out_ref[0:ne, :] += functools.reduce(jnp.add, [g[rows : rows + ne] for g in wide])
        parts = functools.reduce(jnp.add, [g[rows + ne :] for g in wide])
        out_ref[rows : rows + NLOC, :] = (
            parts[0:NLOC] + parts[NLOC : 2 * NLOC] + parts[2 * NLOC : 3 * NLOC]
        )
    mine = pl.ds(pl.multiple_of(core * half, half), half)
    out_ref[mine, :] += sums_ref[mine, :] + shared_ref[0:half, :]
    both = sums_ref[rows : rows + SUB, :] + shared_ref[half : half + SUB, :]
    out_ref[rows : rows + SUB, :] += jnp.where(core == 0, both, jnp.zeros_like(both))


def repack_kernel(mine_ref, theirs_ref, sums_ref, sent_ref, half_ref):
    sums_ref[...] = mine_ref[...] + theirs_ref[...]
    pack(sums_ref, sent_ref, half_ref)


def row_of(x, j):
    return jnp.broadcast_to(x[j : j + 1, :], x.shape)


def eliminate(systems):
    count = len(systems[0][0])
    sub = lax.broadcasted_iota(jnp.int32, (SUB, LANES), 0)
    lane = lax.broadcasted_iota(jnp.int32, (SUB, LANES), 1)
    first = jnp.where(lane < LANES // 2, 0, LANES // 2)

    def step(k, systems):
        at = [first + (SUB * k + j) for j in range(SUB)]
        spread = [
            [
                [jnp.take_along_axis(x, at[j], axis=1, mode="promise_in_bounds") for x in left]
                for j in range(SUB)
            ]
            for left, _ in systems
        ]
        diags = [[col[j][0] for j in range(SUB)] for col in spread]
        panels = [[left[0], right[0]] for left, right in systems]
        scales = [None] * len(systems)
        for j in range(SUB):
            for s, (diag, panel) in enumerate(zip(diags, panels)):
                inverse = 1.0 / row_of(diag[j], j)
                factor = jnp.where(sub == j, 0.0, diag[j]) * inverse
                scales[s] = inverse if j == 0 else jnp.where(sub == j, inverse, scales[s])
                for values, start in ((diag, j + 1), (panel, 0)):
                    for l in range(start, len(values)):
                        values[l] = values[l] - factor * row_of(values[l], j)
        result = []
        for (left, right), panel, scale, col in zip(systems, panels, scales, spread):
            left, right = list(left), list(right)
            panel = [x * scale for x in panel]
            for i in range(1, count):
                for j in range(SUB):
                    left[i] = left[i] - col[j][i] * row_of(panel[0], j)
                    right[i] = right[i] - col[j][i] * row_of(panel[1], j)
            result.append((left[1:] + panel[:1], right[1:] + panel[1:]))
        return result

    return [right for _, right in lax.fori_loop(0, count, step, systems, unroll=2)]


def finish_kernel(
    mine_ref, theirs_ref, anomaly_ref, members_ref, regions_hbm, out_hbm,
    coeff_ref, regions_ref, updated_ref, sems,
):
    half, cells = members_ref.shape
    ne = 2 * half
    count = ne // SUB
    pairs = NLOC // 2
    load = pltpu.make_async_copy(regions_hbm, regions_ref, sems.at[0])
    load.start()

    def total(row, rows=SUB):
        return mine_ref[row : row + rows, :] + theirs_ref[row : row + rows, :]

    lane = lax.broadcasted_iota(jnp.int32, (SUB, LANES), 1)
    sub = lax.broadcasted_iota(jnp.int32, (SUB, LANES), 0)
    tail = total((1 + pairs) * ne)
    triangles = total(0, ne)
    turned = triangles.T
    turned = jnp.concatenate([turned[0:ne], turned[ne : 2 * ne]], axis=1)
    systems = []
    for p in range(pairs):
        diagonal = jnp.broadcast_to(tail[pairs + p : pairs + p + 1], (SUB, LANES))
        damped = diagonal + ((ne - 1.0) + jnp.broadcast_to(tail[p : p + 1], (SUB, LANES)) / ne)
        left, right = [], []
        for i in range(count):
            given = (lane % ne < SUB * i + sub) if p == 0 else (lane % ne > SUB * i + sub)
            here = lane % ne == SUB * i + sub
            block = slice(i * SUB, (i + 1) * SUB)
            gram = jnp.where(given, triangles[block], turned[block])
            left.append(jnp.where(here, damped, gram))
            right.append(total((1 + p) * ne + i * SUB) - jnp.where(here, diagonal, gram))
        systems.append((left, right))
    for p, right in enumerate(eliminate(systems)):
        turned = jnp.concatenate(right, axis=0).T
        coeff_ref[2 * p * ne : 2 * (p + 1) * ne, :] = turned.astype(jnp.bfloat16)
    core = lax.axis_index("mem")
    load.wait()
    stores = []
    for b in range(cells // BLOCK):
        start = pl.multiple_of(regions_ref[b] * ne + core * half, half)
        span = slice(b * BLOCK, (b + 1) * BLOCK)
        delta = jnp.dot(
            coeff_ref[pl.ds(start, half), :], anomaly_ref[:, span], preferred_element_type=jnp.float32
        )
        updated_ref[:, span] = (members_ref[:, span].astype(jnp.float32) + delta).astype(jnp.bfloat16)
        stores.append(
            pltpu.make_async_copy(updated_ref.at[:, span], out_hbm.at[:, span], sems.at[1 + b])
        )
        stores[-1].start()
    for store in stores:
        store.wait()


def anomaly_kernel(mine_ref, theirs_ref, out_ref):
    half = mine_ref.shape[0]
    core = lax.axis_index("mem")
    mine = mine_ref[...].astype(jnp.float32)
    theirs = theirs_ref[...].astype(jnp.float32)
    total = jnp.sum(mine, axis=0, keepdims=True) + jnp.sum(theirs, axis=0, keepdims=True)
    center = total / (2 * half)
    at_mine = pl.ds(pl.multiple_of(core * half, half), half)
    at_theirs = pl.ds(pl.multiple_of((1 - core) * half, half), half)
    out_ref[at_mine, :] = (mine - center).astype(jnp.bfloat16)
    out_ref[at_theirs, :] = (theirs - center).astype(jnp.bfloat16)


def stages(sizes):
    bits = [
        [(axis, 1 << i) for i in range(size.bit_length() - 1)] for axis, size in enumerate(sizes)
    ]
    first, last = bits
    groups = []
    while first or last:
        group = first[:2] + last[:1]
        first, last = first[2:], last[1:]
        groups.append(group)
    return groups


PARTNERS = {1: ((), (), 1), 2: ((1,), (3,), 2), 3: ((4, 3, 2), (5, 7, 6), 1)}


def partners(group, sizes):
    low, high, shared = PARTNERS[len(group)]

    def step(mask):
        way = [0, 0]
        for i, (axis, bit) in enumerate(group):
            if mask >> i & 1:
                way[axis] |= bit
        return way

    def place(c, o, m):
        return (c * sizes[1] + o) * 2 + m

    ways = [(step(a), step(b)) for a, b in zip(low, high)] + [(step(shared), step(shared))]
    return [
        [
            (place(c, o, m), place(c ^ way[m][0], o ^ way[m][1], m))
            for c in range(sizes[0])
            for o in range(sizes[1])
            for m in range(2)
        ]
        for way in ways
    ]


def body(members, observed, obs_error, obs_cells, perturbations, region_ids):
    half, cells = members.shape
    ne = 2 * half
    nobs = observed.shape[0]
    blocks = region_ids.shape[0]
    rows = (1 + NLOC // 2) * ne
    swap = [(0, 1), (1, 0)]
    other = lax.ppermute(members, "mem", swap)
    mine, onehot, predicted, innov, noise, lines = pl.pallas_call(
        prepare_kernel,
        out_shape=[
            pltpu.VMEM((half, cells), jnp.bfloat16),
            pltpu.VMEM((TILE, nobs), jnp.bfloat16),
            pltpu.VMEM((half, nobs), jnp.float32),
            pltpu.VMEM((half, nobs), jnp.bfloat16),
            pltpu.VMEM((half, nobs), jnp.bfloat16),
            pltpu.VMEM((SUB, nobs), jnp.float32),
        ],
        in_specs=[HBM] * 6,
        out_specs=[VMEM] * 6,
        scratch_shapes=[
            pltpu.VMEM((1, nobs), jnp.int32),
            pltpu.VMEM((1, nobs), jnp.float32),
            pltpu.VMEM((1, nobs), jnp.float32),
            pltpu.VMEM((ne, nobs), jnp.bfloat16),
            pltpu.SMEM((blocks,), jnp.int32),
            pltpu.SemaphoreType.DMA((6,)),
        ],
        name="prepare",
    )(
        members,
        obs_cells.reshape(1, nobs),
        observed.reshape(1, nobs),
        obs_error.reshape(1, nobs),
        perturbations.T,
        region_ids,
    )
    sums_shape = pltpu.VMEM((rows + SUB, LANES), jnp.float32)
    packed = [
        sums_shape,
        pltpu.VMEM((rows + ne + 4 * NLOC, LANES), jnp.bfloat16),
        pltpu.VMEM((rows // 2 + SUB, LANES), jnp.float32),
    ]
    sums, sent, shared = pl.pallas_call(
        stats_kernel,
        out_shape=packed,
        in_specs=[VMEM] * 6,
        out_specs=[VMEM] * 3,
        scratch_shapes=[pltpu.VMEM((ne, nobs), jnp.bfloat16)] * 2,
        name="stats",
    )(*[near(x) for x in (other, onehot, predicted, innov, noise, lines)])
    anomaly = pl.pallas_call(
        anomaly_kernel,
        out_shape=pltpu.VMEM((ne, cells), jnp.bfloat16),
        in_specs=[VMEM] * 2,
        out_specs=VMEM,
        name="anomaly",
    )(near(mine), near(other))
    axes = ("cells", "obs", "mem")
    sizes = (lax.axis_size("cells"), lax.axis_size("obs"))
    groups = stages(sizes)
    for number, group in enumerate(groups):
        *single, common = partners(group, sizes)
        got = [lax.ppermute(sent, axes, p) for p in single]
        got.insert(0, lax.ppermute(shared, axes, common))
        if number == 0:
            got, anomaly = lax.optimization_barrier((got, anomaly))
        total = pl.pallas_call(
            fold_kernel,
            out_shape=sums_shape,
            in_specs=[VMEM] * (1 + len(got)),
            out_specs=VMEM,
            name="fold",
        )(near(sums), *[near(g) for g in got])
        theirs = lax.ppermute(total, "mem", swap)
        if number < len(groups) - 1:
            sums, sent, shared = pl.pallas_call(
                repack_kernel,
                out_shape=packed,
                in_specs=[VMEM] * 2,
                out_specs=[VMEM] * 3,
                name="repack",
            )(near(total), near(theirs))
    return pl.pallas_call(
        finish_kernel,
        out_shape=jax.ShapeDtypeStruct((half, cells), jnp.bfloat16),
        in_specs=[VMEM] * 4 + [HBM],
        out_specs=HBM,
        scratch_shapes=[
            pltpu.VMEM((NLOC * ne, ne), jnp.bfloat16),
            pltpu.SMEM((blocks,), jnp.int32),
            pltpu.VMEM((half, cells), jnp.bfloat16),
            pltpu.SemaphoreType.DMA((1 + blocks,)),
        ],
        name="finish",
    )(near(total), near(theirs), near(anomaly), near(mine), region_ids)


def solution(mesh):
    cut = ("groups", "cells", "obs")
    in_specs = (P("mem", cut), P(cut), P(cut), P(cut), P(cut, None), P(cut))
    return jax.shard_map(
        body, mesh=mesh, in_specs=in_specs, out_specs=P("mem", cut), check_vma=False
    )
```

```python
import functools

import jax
import jax.numpy as jnp
from jax import lax
from jax.experimental import pallas as pl
from jax.experimental.pallas import tpu as pltpu
from jax.sharding import PartitionSpec as P

NLOC = 4
BLOCK = 512
SUB = 8
LANES = 128
TILE = 256


VMEM = pl.BlockSpec(memory_space=pltpu.VMEM)
SMEM = pl.BlockSpec(memory_space=pltpu.SMEM)
HBM = pl.BlockSpec(memory_space=pl.ANY)


def near(x):
    return pltpu.with_memory_space_constraint(x, pltpu.VMEM)


def prepare_kernel(
    members_hbm, cells_hbm, observed_hbm, error_hbm, noise_hbm, regions_hbm,
    members_ref, onehot_ref, predicted_ref, innov_ref, noise_ref, rows_ref, cells_ref, observed_ref,
    error_ref, all_noise_ref, regions_ref, sems,
):
    moves = [
        pltpu.make_async_copy(src, dst, sems.at[i])
        for i, (src, dst) in enumerate(
            (
                (cells_hbm, cells_ref),
                (members_hbm, members_ref),
                (error_hbm, error_ref),
                (observed_hbm, observed_ref),
                (noise_hbm, all_noise_ref),
                (regions_hbm, regions_ref),
            )
        )
    ]
    for move in moves:
        move.start()
    half, cells = members_ref.shape
    nobs = cells_ref.shape[1]
    place = lax.broadcasted_iota(jnp.int32, (TILE, LANES), 0).astype(jnp.float32).astype(jnp.bfloat16)
    place = jnp.concatenate([place] * (nobs // LANES), axis=1)
    one = jnp.ones((TILE, nobs), jnp.bfloat16)
    moves[0].wait()
    cell = cells_ref[...]
    part = cell // TILE
    within = (cell - part * TILE).astype(jnp.float32).astype(jnp.bfloat16)
    onehot = jnp.where(place == within, one, jnp.zeros_like(one))
    onehot_ref[...] = onehot
    moves[1].wait()
    predicted = predict(members_ref, onehot, part)
    predicted_ref[...] = predicted
    moves[2].wait()
    moves[3].wait()
    inverse = 1.0 / error_ref[...]
    moves[4].wait()
    core = lax.axis_index("mem")
    noise = all_noise_ref[pl.ds(pl.multiple_of(core * half, half), half), :].astype(jnp.float32)
    innov = (observed_ref[...] - predicted) * inverse + noise
    innov_ref[...] = innov.astype(jnp.bfloat16)
    noise_ref[...] = all_noise_ref[pl.ds(pl.multiple_of((1 - core) * half, half), half), :]
    moves[5].wait()
    block = cell // BLOCK
    region = jnp.zeros_like(cell)
    for b in range(cells // BLOCK):
        region = jnp.where(block == b, regions_ref[b], region)
    rows_ref[0:1, :] = observed_ref[...]
    rows_ref[1:2, :] = inverse
    rows_ref[2:3, :] = part.astype(jnp.float32)
    rows_ref[3:4, :] = region.astype(jnp.float32)
    rows_ref[4:5, :] = jnp.sum(predicted, axis=0, keepdims=True)
    rows_ref[5:6, :] = jnp.sum(innov * innov, axis=0, keepdims=True)
    rows_ref[6:8, :] = jnp.zeros((2, nobs), jnp.float32)


def predict(members_ref, onehot, part):
    members, cells = members_ref.shape
    tiles = cells // TILE
    stacked = jnp.concatenate(
        [members_ref[:, p * TILE : (p + 1) * TILE] for p in range(tiles)], axis=0
    )
    picked = jnp.dot(stacked, onehot, preferred_element_type=jnp.float32)
    values = picked[0:members]
    for p in range(1, tiles):
        values = jnp.where(part == p, picked[p * members : (p + 1) * members], values)
    return values + 0.2 * values * values * values


def stats_kernel(
    theirs_ref, onehot_ref, predicted_ref, innov_ref, noise_ref, rows_ref,
    sums_ref, sent_ref, half_ref, sens_ref, innovs_ref,
):
    half = theirs_ref.shape[0]
    ne = 2 * half
    pairs = NLOC // 2
    core = lax.axis_index("mem")
    at_mine = pl.ds(pl.multiple_of(core * half, half), half)
    at_theirs = pl.ds(pl.multiple_of((1 - core) * half, half), half)
    observed, inverse, part, region, mine_sum, mine_square = [rows_ref[i : i + 1, :] for i in range(6)]
    mine = predicted_ref[...]
    theirs = predict(theirs_ref, onehot_ref[...], part)
    innov = (observed - theirs) * inverse + noise_ref[...].astype(jnp.float32)
    square = mine_square + jnp.sum(innov * innov, axis=0, keepdims=True)
    pmean = (mine_sum + jnp.sum(theirs, axis=0, keepdims=True)) / ne
    sens_ref[at_mine, :] = ((mine - pmean) * inverse).astype(jnp.bfloat16)
    sens_ref[at_theirs, :] = ((theirs - pmean) * inverse).astype(jnp.bfloat16)
    innovs_ref[at_mine, :] = innov_ref[...]
    innovs_ref[at_theirs, :] = innov.astype(jnp.bfloat16)
    sens = sens_ref[...]
    inside = [region == r for r in range(NLOC)]
    lane = lax.broadcasted_iota(jnp.int32, (SUB, LANES), 1)
    column = lax.broadcasted_iota(jnp.int32, (ne, LANES), 1) % ne
    below = column < lax.broadcasted_iota(jnp.int32, (ne, LANES), 0)
    on_diagonal = column == lax.broadcasted_iota(jnp.int32, (ne, LANES), 0)

    def product(x):
        masked = jnp.concatenate([jnp.where(m, x, jnp.zeros_like(x)) for m in inside], axis=0)
        return lax.dot_general(
            sens, masked, (((1,), (1,)), ((), ())), preferred_element_type=jnp.float32
        )

    gram = product(sens)
    cross = product(innovs_ref[...])
    misfits = [
        jnp.sum(jnp.where(m, square, jnp.float32(0.0)), axis=1, keepdims=True) for m in inside
    ]
    for p in range(pairs):
        lanes = slice(p * LANES, (p + 1) * LANES)
        g = gram[:, lanes]
        row = (1 + p) * ne
        sums_ref[row : row + ne, :] = cross[:, lanes] + g
        tail = (1 + pairs) * ne
        sums_ref[tail + p : tail + p + 1, :] = jnp.where(
            lane < ne, misfits[2 * p], misfits[2 * p + 1]
        )[0:1]
        sums_ref[tail + pairs + p : tail + pairs + p + 1, :] = jnp.sum(
            jnp.where(on_diagonal, g, 0.0), axis=0, keepdims=True
        )
    sums_ref[0:ne, :] = jnp.where(
        on_diagonal, 0.0, jnp.where(below, gram[:, 0:LANES], gram[:, LANES : 2 * LANES])
    )
    sums_ref[tail + 2 * pairs : tail + SUB, :] = jnp.zeros((SUB - 2 * pairs, LANES), jnp.float32)
    pack(sums_ref, sent_ref, half_ref)


def pack(sums_ref, sent_ref, half_ref):
    rows = sums_ref.shape[0] - SUB
    ne = rows // (1 + NLOC // 2)
    sent_ref[0:rows, :] = sums_ref[0:rows, :].astype(jnp.bfloat16)
    triangles = sums_ref[0:ne, :]
    rest = triangles - triangles.astype(jnp.bfloat16).astype(jnp.float32)
    sent_ref[rows : rows + ne, :] = rest.astype(jnp.bfloat16)
    left = sums_ref[rows : rows + NLOC, :]
    parts = []
    for _ in range(3):
        part = left.astype(jnp.bfloat16).astype(jnp.float32)
        parts.append(part)
        left = left - part
    parts.append(jnp.zeros_like(left))
    sent_ref[rows + ne : rows + ne + 4 * NLOC, :] = jnp.concatenate(parts, axis=0).astype(jnp.bfloat16)
    pick_half(sums_ref, half_ref)


def pick_half(sums_ref, half_ref):
    rows = sums_ref.shape[0] - SUB
    half = rows // 2
    start = pl.multiple_of(lax.axis_index("mem") * half, half)
    half_ref[0:half, :] = sums_ref[pl.ds(start, half), :]
    half_ref[half : half + SUB, :] = sums_ref[rows : rows + SUB, :]


def fold_kernel(*refs):
    sums_ref, shared_ref, *got, out_ref = refs
    rows = sums_ref.shape[0] - SUB
    half = rows // 2
    core = lax.axis_index("mem")
    ne = rows // (1 + NLOC // 2)
    out_ref[...] = jnp.zeros_like(out_ref)
    if got:
        wide = [g[...].astype(jnp.float32) for g in got]
        out_ref[0:rows, :] = functools.reduce(jnp.add, [g[0:rows] for g in wide])
        out_ref[0:ne, :] += functools.reduce(jnp.add, [g[rows : rows + ne] for g in wide])
        parts = functools.reduce(jnp.add, [g[rows + ne :] for g in wide])
        out_ref[rows : rows + NLOC, :] = (
            parts[0:NLOC] + parts[NLOC : 2 * NLOC] + parts[2 * NLOC : 3 * NLOC]
        )
    mine = pl.ds(pl.multiple_of(core * half, half), half)
    out_ref[mine, :] += sums_ref[mine, :] + shared_ref[0:half, :]
    both = sums_ref[rows : rows + SUB, :] + shared_ref[half : half + SUB, :]
    out_ref[rows : rows + SUB, :] += jnp.where(core == 0, both, jnp.zeros_like(both))


def repack_kernel(mine_ref, theirs_ref, sums_ref, sent_ref, half_ref):
    sums_ref[...] = mine_ref[...] + theirs_ref[...]
    pack(sums_ref, sent_ref, half_ref)


def row_of(x, j):
    return jnp.broadcast_to(x[j : j + 1, :], x.shape)


def eliminate(systems):
    count = len(systems[0][0])
    sub = lax.broadcasted_iota(jnp.int32, (SUB, LANES), 0)
    lane = lax.broadcasted_iota(jnp.int32, (SUB, LANES), 1)
    first = jnp.where(lane < LANES // 2, 0, LANES // 2)

    def step(k, systems):
        at = [first + (SUB * k + j) for j in range(SUB)]
        spread = [
            [
                [jnp.take_along_axis(x, at[j], axis=1, mode="promise_in_bounds") for x in left]
                for j in range(SUB)
            ]
            for left, _ in systems
        ]
        diags = [[col[j][0] for j in range(SUB)] for col in spread]
        panels = [[left[0], right[0]] for left, right in systems]
        scales = [None] * len(systems)
        for j in range(SUB):
            for s, (diag, panel) in enumerate(zip(diags, panels)):
                inverse = 1.0 / row_of(diag[j], j)
                factor = jnp.where(sub == j, 0.0, diag[j]) * inverse
                scales[s] = inverse if j == 0 else jnp.where(sub == j, inverse, scales[s])
                for values, start in ((diag, j + 1), (panel, 0)):
                    for l in range(start, len(values)):
                        values[l] = values[l] - factor * row_of(values[l], j)
        result = []
        for (left, right), panel, scale, col in zip(systems, panels, scales, spread):
            left, right = list(left), list(right)
            panel = [x * scale for x in panel]
            for i in range(1, count):
                for j in range(SUB):
                    left[i] = left[i] - col[j][i] * row_of(panel[0], j)
                    right[i] = right[i] - col[j][i] * row_of(panel[1], j)
            result.append((left[1:] + panel[:1], right[1:] + panel[1:]))
        return result

    return [right for _, right in lax.fori_loop(0, count, step, systems, unroll=2)]


def finish_kernel(
    mine_ref, theirs_ref, anomaly_ref, members_ref, regions_hbm, out_hbm,
    coeff_ref, regions_ref, updated_ref, sems,
):
    half, cells = members_ref.shape
    ne = 2 * half
    count = ne // SUB
    pairs = NLOC // 2
    load = pltpu.make_async_copy(regions_hbm, regions_ref, sems.at[0])
    load.start()

    def total(row, rows=SUB):
        return mine_ref[row : row + rows, :] + theirs_ref[row : row + rows, :]

    lane = lax.broadcasted_iota(jnp.int32, (SUB, LANES), 1)
    sub = lax.broadcasted_iota(jnp.int32, (SUB, LANES), 0)
    tail = total((1 + pairs) * ne)
    triangles = total(0, ne)
    turned = triangles.T
    turned = jnp.concatenate([turned[0:ne], turned[ne : 2 * ne]], axis=1)
    systems = []
    for p in range(pairs):
        diagonal = jnp.broadcast_to(tail[pairs + p : pairs + p + 1], (SUB, LANES))
        damped = diagonal + ((ne - 1.0) + jnp.broadcast_to(tail[p : p + 1], (SUB, LANES)) / ne)
        left, right = [], []
        for i in range(count):
            given = (lane % ne < SUB * i + sub) if p == 0 else (lane % ne > SUB * i + sub)
            here = lane % ne == SUB * i + sub
            block = slice(i * SUB, (i + 1) * SUB)
            gram = jnp.where(given, triangles[block], turned[block])
            left.append(jnp.where(here, damped, gram))
            right.append(total((1 + p) * ne + i * SUB) - jnp.where(here, diagonal, gram))
        systems.append((left, right))
    for p, right in enumerate(eliminate(systems)):
        turned = jnp.concatenate(right, axis=0).T
        coeff_ref[2 * p * ne : 2 * (p + 1) * ne, :] = turned.astype(jnp.bfloat16)
    core = lax.axis_index("mem")
    load.wait()
    stores = []
    for b in range(cells // BLOCK):
        start = pl.multiple_of(regions_ref[b] * ne + core * half, half)
        span = slice(b * BLOCK, (b + 1) * BLOCK)
        delta = jnp.dot(
            coeff_ref[pl.ds(start, half), :], anomaly_ref[:, span], preferred_element_type=jnp.float32
        )
        updated_ref[:, span] = (members_ref[:, span].astype(jnp.float32) + delta).astype(jnp.bfloat16)
        stores.append(
            pltpu.make_async_copy(updated_ref.at[:, span], out_hbm.at[:, span], sems.at[1 + b])
        )
        stores[-1].start()
    for store in stores:
        store.wait()


def anomaly_kernel(mine_ref, theirs_ref, out_ref):
    half = mine_ref.shape[0]
    core = lax.axis_index("mem")
    mine = mine_ref[...].astype(jnp.float32)
    theirs = theirs_ref[...].astype(jnp.float32)
    total = jnp.sum(mine, axis=0, keepdims=True) + jnp.sum(theirs, axis=0, keepdims=True)
    center = total / (2 * half)
    at_mine = pl.ds(pl.multiple_of(core * half, half), half)
    at_theirs = pl.ds(pl.multiple_of((1 - core) * half, half), half)
    out_ref[at_mine, :] = (mine - center).astype(jnp.bfloat16)
    out_ref[at_theirs, :] = (theirs - center).astype(jnp.bfloat16)


def stages(sizes):
    bits = [
        [(axis, 1 << i) for i in range(size.bit_length() - 1)] for axis, size in enumerate(sizes)
    ]
    first, last = bits
    groups = []
    while first or last:
        group = first[:2] + last[:1]
        first, last = first[2:], last[1:]
        groups.append(group)
    return groups


PARTNERS = {1: ((), (), 1), 2: ((1,), (3,), 2), 3: ((4, 5, 3), (1, 6, 7), 2)}


def partners(group, sizes):
    low, high, shared = PARTNERS[len(group)]

    def step(mask):
        way = [0, 0]
        for i, (axis, bit) in enumerate(group):
            if mask >> i & 1:
                way[axis] |= bit
        return way

    def place(c, o, m):
        return (c * sizes[1] + o) * 2 + m

    ways = [(step(a), step(b)) for a, b in zip(low, high)] + [(step(shared), step(shared))]
    return [
        [
            (place(c, o, m), place(c ^ way[m][0], o ^ way[m][1], m))
            for c in range(sizes[0])
            for o in range(sizes[1])
            for m in range(2)
        ]
        for way in ways
    ]


def body(members, observed, obs_error, obs_cells, perturbations, region_ids):
    half, cells = members.shape
    ne = 2 * half
    nobs = observed.shape[0]
    blocks = region_ids.shape[0]
    rows = (1 + NLOC // 2) * ne
    swap = [(0, 1), (1, 0)]
    other = lax.ppermute(members, "mem", swap)
    mine, onehot, predicted, innov, noise, lines = pl.pallas_call(
        prepare_kernel,
        out_shape=[
            pltpu.VMEM((half, cells), jnp.bfloat16),
            pltpu.VMEM((TILE, nobs), jnp.bfloat16),
            pltpu.VMEM((half, nobs), jnp.float32),
            pltpu.VMEM((half, nobs), jnp.bfloat16),
            pltpu.VMEM((half, nobs), jnp.bfloat16),
            pltpu.VMEM((SUB, nobs), jnp.float32),
        ],
        in_specs=[HBM] * 6,
        out_specs=[VMEM] * 6,
        scratch_shapes=[
            pltpu.VMEM((1, nobs), jnp.int32),
            pltpu.VMEM((1, nobs), jnp.float32),
            pltpu.VMEM((1, nobs), jnp.float32),
            pltpu.VMEM((ne, nobs), jnp.bfloat16),
            pltpu.SMEM((blocks,), jnp.int32),
            pltpu.SemaphoreType.DMA((6,)),
        ],
        name="prepare",
    )(
        members,
        obs_cells.reshape(1, nobs),
        observed.reshape(1, nobs),
        obs_error.reshape(1, nobs),
        perturbations.T,
        region_ids,
    )
    sums_shape = pltpu.VMEM((rows + SUB, LANES), jnp.float32)
    packed = [
        sums_shape,
        pltpu.VMEM((rows + ne + 4 * NLOC, LANES), jnp.bfloat16),
        pltpu.VMEM((rows // 2 + SUB, LANES), jnp.float32),
    ]
    sums, sent, shared = pl.pallas_call(
        stats_kernel,
        out_shape=packed,
        in_specs=[VMEM] * 6,
        out_specs=[VMEM] * 3,
        scratch_shapes=[pltpu.VMEM((ne, nobs), jnp.bfloat16)] * 2,
        name="stats",
    )(*[near(x) for x in (other, onehot, predicted, innov, noise, lines)])
    anomaly = pl.pallas_call(
        anomaly_kernel,
        out_shape=pltpu.VMEM((ne, cells), jnp.bfloat16),
        in_specs=[VMEM] * 2,
        out_specs=VMEM,
        name="anomaly",
    )(near(mine), near(other))
    axes = ("cells", "obs", "mem")
    sizes = (lax.axis_size("cells"), lax.axis_size("obs"))
    groups = stages(sizes)
    for number, group in enumerate(groups):
        *single, common = partners(group, sizes)
        got = [lax.ppermute(sent, axes, p) for p in single]
        got.insert(0, lax.ppermute(shared, axes, common))
        if number == 0:
            got, anomaly = lax.optimization_barrier((got, anomaly))
        total = pl.pallas_call(
            fold_kernel,
            out_shape=sums_shape,
            in_specs=[VMEM] * (1 + len(got)),
            out_specs=VMEM,
            name="fold",
        )(near(sums), *[near(g) for g in got])
        theirs = lax.ppermute(total, "mem", swap)
        if number < len(groups) - 1:
            sums, sent, shared = pl.pallas_call(
                repack_kernel,
                out_shape=packed,
                in_specs=[VMEM] * 2,
                out_specs=[VMEM] * 3,
                name="repack",
            )(near(total), near(theirs))
    return pl.pallas_call(
        finish_kernel,
        out_shape=jax.ShapeDtypeStruct((half, cells), jnp.bfloat16),
        in_specs=[VMEM] * 4 + [HBM],
        out_specs=HBM,
        scratch_shapes=[
            pltpu.VMEM((NLOC * ne, ne), jnp.bfloat16),
            pltpu.SMEM((blocks,), jnp.int32),
            pltpu.VMEM((half, cells), jnp.bfloat16),
            pltpu.SemaphoreType.DMA((1 + blocks,)),
        ],
        name="finish",
    )(near(total), near(theirs), near(anomaly), near(mine), region_ids)


def solution(mesh):
    cut = ("groups", "cells", "obs")
    in_specs = (P("mem", cut), P(cut), P(cut), P(cut), P(cut, None), P(cut))
    return jax.shard_map(
        body, mesh=mesh, in_specs=in_specs, out_specs=P("mem", cut), check_vma=False
    )
```
